128 devices in a mesh: dom: 128 (over z, x, y, core).
Axes of the slice: x: 4, y: 4, z: 4, core: 2. Of those that a mesh axis runs over, the one named last changes fastest.
Arguments:
- field: float32 [3, 720896], P(None, 'dom'), may hold values from -6 to 6
- blocks: bfloat16 [30, 30, 524288], P(None, None, 'dom'), may hold values from -1 to 1
- connectivity: int32 [10, 524288], P(None, 'dom'), may hold values from 0 to 8703, as said below
- send_nodes: int32 [8, 49152], P(None, 'dom'), may hold values from 0 to 5631
- live_blocks: int32 [128], replicated, may hold values from 1 to 8
Outputs:
- image: float32 [3, 720896], P(None, 'dom')
The draws below stay inside these ranges and needn't reach their ends.
Inputs may be any that keep to these rules, and one draw needn't show every extreme that they name: `connectivity`: entries below 5632 name nodes of the element's own subdomain; entry 5632 + k * 384 + g names the node sent as entry g of row k by subdomain d - o_k, and only where that subdomain exists. `send_nodes`: columns d * 384 to (d + 1) * 384 - 1 of row k list local indices of nodes that subdomain d owns, in the order in which subdomain d + o_k numbers its ghost slots from d. Subdomain d's elements fill its first 512 * live_blocks[d] slots; the other slots are unused.
All inputs are finite; a program needn't handle non-finite values.
Results may differ from the reference program's by a relative error of at most 0.0003.
Values sent between devices are 32-bit elements; how exact they have to be, the bound alone decides.
No kernel may reach another device: no remote copies, remote signals or barrier semaphores. Data moves between devices by JAX's collectives and lax.ppermute only.
A program may use at most 64 MiB of HBM per device.

```python
import jax
import jax.numpy as jnp
from jax import lax

ELEM_DEV = 4096
BLK = 512
REACH = 4
NODE_DEV = 5632
GHOST = 384
NBLK = 8
NODES = 720896
ELEMS = 524288
N_DOM = 128


def draw_connectivity(key, part):
    slot_total = N_DOM * ELEM_DEV
    key_local, key_ghost, key_pick = jax.random.split(jax.random.fold_in(key, 11), 3)
    local_ids = jax.random.randint(key_local, (10, slot_total), 0, NODE_DEV)
    ghost_ids = jax.random.randint(key_ghost, (10, slot_total), 0, 2 * REACH * GHOST)
    picked = jax.random.randint(key_pick, (10, slot_total), 0, 5) == 0
    device = jnp.arange(slot_total, dtype=jnp.int32)[None, :] // ELEM_DEV
    bucket = ghost_ids // GHOST
    offset = jnp.where(bucket < REACH, bucket + 1, REACH - 1 - bucket)
    source = device - offset
    usable = picked & (source >= 0) & (source < N_DOM)
    return jnp.where(usable, NODE_DEV + ghost_ids, local_ids).astype(jnp.int32)


def plant(values, key, low, high):
    spot = [jax.random.randint(jax.random.fold_in(key, axis), (), 0, length) for axis, length in enumerate(values.shape)]
    longest = values.shape.index(max(values.shape))
    beside = spot[:longest] + [(spot[longest] + 1) % values.shape[longest]] + spot[longest + 1:]
    return values.at[tuple(spot)].set(low).at[tuple(beside)].set(high)


def block_scale(stream_key, shape, cuts, smallest, high):
    factor_of, own = 1.0, jax.random.fold_in(stream_key, 6)
    for position, shards_of in cuts:
        steps = jnp.exp(jax.random.uniform(jax.random.fold_in(own, position), (shards_of,), jnp.float32, smallest / len(cuts), high / len(cuts)))
        factor_of = factor_of * jnp.repeat(steps, shape[position] // shards_of).reshape([-1 if axis == position else 1 for axis in range(len(shape))])
    return factor_of


def noise(stream_key, dims, scale, most, shards=(), kind=jnp.bfloat16):
    gain = block_scale(stream_key, dims, shards, -0.22, 0.18) if shards else 1.0
    drawn = jax.random.normal(stream_key, dims, jnp.float32) * scale * gain
    return jnp.minimum(jnp.maximum(drawn, -most), most).astype(kind)


def setup_inputs(seed: int = 0) -> dict:
    arg_keys = jax.random.split(jax.random.key(seed), 6)
    field = noise(arg_keys[0], (3, NODES), 1.0, 6.0, ((1, 128),), jnp.float32)
    blocks = noise(arg_keys[1], (30, 30, ELEMS), 30 ** -0.5, 1.0, ((2, 128),))
    connectivity = draw_connectivity(jax.random.fold_in(arg_keys[5], 71), 0)
    send_nodes = plant(jax.random.randint(arg_keys[3], (2 * REACH, N_DOM * GHOST), 0, NODE_DEV), jax.random.fold_in(arg_keys[3], 1), 0, NODE_DEV - 1).astype(jnp.int32)
    live_blocks = plant(jax.random.randint(arg_keys[4], (N_DOM,), NBLK // 8, NBLK + 1), jax.random.fold_in(arg_keys[4], 1), NBLK // 8, NBLK).astype(jnp.int32)
    return {"field": field, "blocks": blocks, "connectivity": connectivity, "send_nodes": send_nodes, "live_blocks": live_blocks}


def reference(field, blocks, connectivity, send_nodes, live_blocks):
    node_total = N_DOM * NODE_DEV
    offsets = jnp.array([k + 1 if k < REACH else REACH - 1 - k for k in range(2 * REACH)], jnp.int32)
    padded = jnp.concatenate([field, jnp.zeros((3, 1), field.dtype)], axis=1)

    def partition_step(totals, device):
        local_ids = device * NODE_DEV + jnp.arange(NODE_DEV, dtype=jnp.int32)
        pieces = [local_ids]
        for k in range(2 * REACH):
            source = device - offsets[k]
            inside = (source >= 0) & (source < N_DOM)
            clipped = jnp.clip(source, 0, N_DOM - 1).astype(jnp.int32)
            sent_rows = lax.dynamic_slice_in_dim(send_nodes[k], clipped * GHOST, GHOST)
            pieces.append(jnp.where(inside, clipped * NODE_DEV + sent_rows, node_total).astype(jnp.int32))
        global_ids = jnp.concatenate(pieces)
        element_nodes = lax.dynamic_slice_in_dim(connectivity, (device * ELEM_DEV).astype(jnp.int32), ELEM_DEV, 1)
        node_ids = global_ids[element_nodes]
        values = padded[:, node_ids].reshape(30, ELEM_DEV)
        stiffness = lax.dynamic_slice_in_dim(blocks, (device * ELEM_DEV).astype(jnp.int32), ELEM_DEV, 2).astype(jnp.float32)
        forces = jnp.einsum("ije,je->ie", stiffness, values, precision=lax.Precision.HIGHEST)
        live_mask = jnp.arange(ELEM_DEV, dtype=jnp.int32) < live_blocks[device] * BLK
        forces = jnp.where(live_mask[None, :], forces, 0.0)
        totals = totals.at[:, node_ids.reshape(-1)].add(forces.reshape(3, 10 * ELEM_DEV))
        return totals, None

    totals = jnp.zeros((3, node_total + 1), jnp.float32)
    totals, _ = lax.scan(partition_step, totals, jnp.arange(N_DOM, dtype=jnp.int32))
    return totals[:, :node_total]
```

```python
import jax
import jax.numpy as jnp
from jax import lax
from jax.experimental import pallas as pl
from jax.experimental.pallas import tpu as pltpu
from jax.sharding import PartitionSpec as P

F32 = jnp.float32
BF16 = jnp.bfloat16
LANES = 128
WIDE = 256
BLK = 512
ELEMS = 4096
NBLK = ELEMS // BLK
NODES = 5632
GHOST = 384
SLOTS = NODES + 8 * GHOST
OWN_ROWS = NODES // WIDE
ALL_ROWS = SLOTS // WIDE
TILES = BLK // LANES
VMEM = pl.BlockSpec(memory_space=pltpu.VMEM)


def pad16(n):
    return -(-n // 16) * 16


def iota_rows(rows):
    return lax.broadcasted_iota(jnp.int32, (rows, LANES), 0)


def row_upper(rows):
    q = iota_rows(pad16(6 * rows))
    u = q
    for s in range(1, 6):
        u = jnp.where(q >= s * rows, q - s * rows, u)
    return jnp.where(q >= 6 * rows, -1, u)


def one_hot(const_ref, row):
    n = const_ref.shape[0]
    wide = jnp.broadcast_to(row, (16, LANES)).astype(BF16)
    out = []
    for g in range(n // 16):
        out.append(jnp.where(const_ref[pl.ds(16 * g, 16), :] == wide, jnp.ones((), BF16), jnp.zeros((), BF16)))
    return jnp.concatenate(out, axis=0)


def split(x):
    hi = x.astype(BF16).astype(F32)
    return hi, x - hi


def placed(const_ref, row, parts, rows):
    wide = jnp.broadcast_to(row, (16, LANES)).astype(BF16)
    vals = [jnp.broadcast_to(p, (16, LANES)).astype(BF16) for p in parts]
    sub = lax.broadcasted_iota(jnp.int32, (16, LANES), 0)
    zero = jnp.zeros((16, LANES), BF16)
    out = []
    for g in range(const_ref.shape[0] // 16):
        first, last = 16 * g // rows, (16 * g + 15) // rows
        value = vals[min(first, 5)]
        if last != first and last <= 5:
            cut = (first + 1) * rows - 16 * g
            value = jnp.where((sub < cut).astype(F32).astype(BF16) > 0, value, vals[last])
        out.append(jnp.where(const_ref[pl.ds(16 * g, 16), :] == wide, value, zero))
    return jnp.concatenate(out, axis=0)


def pick_kernel(field_ref, send_ref, plus_ref, minus_ref, near_ref):
    place = {1: (plus_ref, 0), 2: (plus_ref, 9), 3: (plus_ref, 18), 5: (minus_ref, 0), 6: (minus_ref, 9), 7: (minus_ref, 18),
             0: (near_ref, 0), 4: (near_ref, 9)}
    for j in range(3):
        index = send_ref[:, pl.ds(j * LANES, LANES)]
        upper, lower = index >> 7, index & 127
        total = [jnp.zeros((8, LANES), F32) for _ in range(3)]
        for h in range(NODES // LANES):
            hit = upper == h
            for c in range(3):
                row = jnp.broadcast_to(field_ref[pl.ds(c, 1), pl.ds(h * LANES, LANES)], (8, LANES))
                total[c] = jnp.where(hit, jnp.take_along_axis(row, lower, axis=1), total[c])
        for c in range(3):
            for k in range(8):
                ref, base = place[k]
                ref[pl.ds(base + c * 3 + j, 1), :] = total[c][k:k + 1, :]


def main_kernel(live_ref, field_ref, aplus_ref, aminus_ref, bplus_ref, bminus_ref, conn_ref, blocks_ref,
                own_ref, mone_ref, pone_ref, own2_ref, own6_ref,
                stiff, sem, tf, table, upper_f, upper_b, lower_b, lo, up, hot, vals, force, put, total):
    n = live_ref[0]

    def fetch(b):
        cols = pl.ds(pl.multiple_of(b * BLK, BLK), BLK)
        return pltpu.make_async_copy(blocks_ref.at[:, :, cols], stiff.at[b], sem.at[b])

    def start(b, _):
        fetch(b).start()
        return 0

    lax.fori_loop(0, n, start, 0)

    ru = row_upper(ALL_ROWS).astype(F32)
    upper_f[...] = ru
    upper_b[...] = ru.astype(BF16)
    lower_b[...] = iota_rows(WIDE).astype(F32).astype(BF16)

    tf[pl.ds(200, 8), :] = jnp.zeros((8, WIDE), F32)

    def fill(x, c, h):
        hi, low = split(x)
        for part, y in ((0, hi), (1, low)):
            tf[pl.ds((c * 2 + part) * ALL_ROWS + h // 2, 1), pl.ds((h % 2) * LANES, LANES)] = y

    for h in range(NODES // LANES):
        x = field_ref[:, pl.ds(h * LANES, LANES)]
        for c in range(3):
            fill(x[c:c + 1, :], c, h)
    source = {2: (aplus_ref, 9), 6: (aminus_ref, 9), 0: (bplus_ref, 0), 3: (bplus_ref, 9), 5: (bplus_ref, 18),
              4: (bminus_ref, 0), 1: (bminus_ref, 9), 7: (bminus_ref, 18)}
    for k in range(8):
        ref, base = source[k]
        for c in range(3):
            for j in range(3):
                fill(ref[pl.ds(base + c * 3 + j, 1), :], c, NODES // LANES + 3 * k + j)
    table[...] = tf[...].astype(BF16)
    total[...] = jnp.zeros_like(total)

    def step(b, _):
        index = conn_ref[:, pl.ds(pl.multiple_of(b * BLK, BLK), BLK)]
        lo[...] = (index & (WIDE - 1)).astype(F32)
        up[...] = (index >> 8).astype(F32)
        for a in range(10):
            for t2 in range(TILES // 2):
                at = (a * TILES + 2 * t2) * LANES
                for s in range(2):
                    row = lo[pl.ds(a, 1), pl.ds((2 * t2 + s) * LANES, LANES)]
                    hot[:, pl.ds(at + s * LANES, LANES)] = one_hot(lower_b, row)
                got = jnp.dot(table[...], hot[:, pl.ds(at, WIDE)], preferred_element_type=F32)
                for s in range(2):
                    row = jnp.broadcast_to(up[pl.ds(a, 1), pl.ds((2 * t2 + s) * LANES, LANES)], (8, LANES))
                    sums = [None, None, None]
                    for g in range(26):
                        hit = jnp.where(upper_f[pl.ds(8 * g, 8), :] == row,
                                        got[8 * g:8 * g + 8, s * LANES:(s + 1) * LANES], 0.0)
                        if g == 8:
                            head = iota_rows(8) < 4
                            sums[0] = sums[0] + jnp.where(head, hit, 0.0)
                            sums[1] = jnp.where(head, 0.0, hit)
                        else:
                            c = 0 if g < 8 else (1 if g < 17 else 2)
                            sums[c] = hit if sums[c] is None else sums[c] + hit
                    for c in range(3):
                        vals[pl.ds(c * 10 + a, 1), pl.ds((2 * t2 + s) * LANES, LANES)] = jnp.sum(sums[c], axis=0, keepdims=True)
        fetch(b).wait()
        for t in range(TILES):
            v = vals[:, pl.ds(t * LANES, LANES)]
            for i in range(30):
                k = stiff[b, i, :, pl.ds(t * LANES, LANES)].astype(F32)
                force[pl.ds(i, 1), pl.ds(t * LANES, LANES)] = jnp.sum(k * v, axis=0, keepdims=True)
        for a in range(10):
            for t in range(TILES):
                parts = []
                for c in range(3):
                    parts.extend(split(force[pl.ds(c * 10 + a, 1), pl.ds(t * LANES, LANES)]))
                row = up[pl.ds(a, 1), pl.ds(t * LANES, LANES)]
                put[:, pl.ds((a * TILES + t) * LANES, LANES)] = placed(upper_b, row, parts, ALL_ROWS)
        total[...] += lax.dot_general(put[...], hot[...], (((1,), (1,)), ((), ())), preferred_element_type=F32)
        return 0

    lax.fori_loop(0, n, step, 0)

    for c in range(3):
        base = 2 * c * ALL_ROWS
        own_ref[pl.ds(c * OWN_ROWS, OWN_ROWS), :] = total[pl.ds(base, OWN_ROWS), :] + total[pl.ds(base + ALL_ROWS, OWN_ROWS), :]
    target = {0: (mone_ref, 0), 3: (mone_ref, 9), 5: (mone_ref, 18), 4: (pone_ref, 0), 1: (pone_ref, 9), 7: (pone_ref, 18),
              2: (own2_ref, 0), 6: (own6_ref, 0)}
    for k in range(8):
        ref, base = target[k]
        for c in range(3):
            for j in range(3):
                h = NODES // LANES + 3 * k + j
                at = 2 * c * ALL_ROWS + h // 2
                cols = pl.ds((h % 2) * LANES, LANES)
                ref[pl.ds(base + c * 3 + j, 1), :] = total[pl.ds(at, 1), cols] + total[pl.ds(at + ALL_ROWS, 1), cols]


def spread_kernel(own_ref, mone_ref, pone_ref, mthree_ref, pthree_ref, send_ref, out_ref, upper_b, lower_b, lo, up, hot, put):
    upper_b[...] = row_upper(OWN_ROWS).astype(F32).astype(BF16)
    lower_b[...] = iota_rows(WIDE).astype(F32).astype(BF16)
    index = send_ref[...]
    lo[...] = (index & (WIDE - 1)).astype(F32)
    up[...] = (index >> 8).astype(F32)
    source = {0: (mone_ref, 0), 4: (pone_ref, 0), 3: (mthree_ref, 0), 2: (mthree_ref, 9), 1: (mthree_ref, 18),
              5: (pthree_ref, 0), 6: (pthree_ref, 9), 7: (pthree_ref, 18)}
    for k in range(8):
        ref, base = source[k]
        for j in range(3):
            at = pl.ds((3 * k + j) * LANES, LANES)
            cols = pl.ds(j * LANES, LANES)
            hot[:, at] = one_hot(lower_b, lo[pl.ds(k, 1), cols])
            parts = []
            for c in range(3):
                parts.extend(split(ref[pl.ds(base + c * 3 + j, 1), :]))
            put[:, at] = placed(upper_b, up[pl.ds(k, 1), cols], parts, OWN_ROWS)
    total = lax.dot_general(put[...], hot[...], (((1,), (1,)), ((), ())), preferred_element_type=F32)
    for c in range(3):
        for u in range(OWN_ROWS):
            q = 2 * c * OWN_ROWS + u
            out_ref[pl.ds(c, 1), pl.ds(u * WIDE, WIDE)] = (
                total[q:q + 1, :] + total[q + OWN_ROWS:q + OWN_ROWS + 1, :] + own_ref[pl.ds(c * OWN_ROWS + u, 1), :]
            )


def shift(x, o):
    n = lax.axis_size("dom")
    return lax.ppermute(x, "dom", [(i, (i + o) % n) for i in range(n)])


def body(field, blocks, connectivity, send_nodes, live_blocks):
    live = lax.dynamic_slice_in_dim(live_blocks, lax.axis_index("dom"), 1)
    f = lambda *s: jax.ShapeDtypeStruct(s, F32)
    plus, minus, near = pl.pallas_call(
        pick_kernel, out_shape=(f(27, LANES), f(27, LANES), f(18, LANES)), in_specs=[VMEM] * 2, out_specs=(VMEM,) * 3, name="pick",
    )(field, send_nodes)
    aplus = shift(plus, 3)
    aminus = shift(minus, -3)
    bplus = shift(jnp.concatenate([near[:9], aplus[18:], aminus[:9]]), 1)
    bminus = shift(jnp.concatenate([near[9:], aplus[:9], aminus[18:]]), -1)
    rows = pad16(6 * ALL_ROWS)
    own, mone, pone, own2, own6 = pl.pallas_call(
        main_kernel,
        out_shape=(f(3 * OWN_ROWS, WIDE), f(27, LANES), f(27, LANES), f(9, LANES), f(9, LANES)),
        in_specs=[pl.BlockSpec(memory_space=pltpu.SMEM)] + [VMEM] * 6 + [pl.BlockSpec(memory_space=pl.ANY)],
        out_specs=(VMEM,) * 5,
        scratch_shapes=[
            pltpu.VMEM((NBLK, 30, 30, BLK), BF16),
            pltpu.SemaphoreType.DMA((NBLK,)),
            pltpu.VMEM((rows, WIDE), F32),
            pltpu.VMEM((rows, WIDE), BF16),
            pltpu.VMEM((rows, LANES), F32),
            pltpu.VMEM((rows, LANES), BF16),
            pltpu.VMEM((WIDE, LANES), BF16),
            pltpu.VMEM((10, BLK), F32),
            pltpu.VMEM((10, BLK), F32),
            pltpu.VMEM((WIDE, 10 * BLK), BF16),
            pltpu.VMEM((30, BLK), F32),
            pltpu.VMEM((30, BLK), F32),
            pltpu.VMEM((rows, 10 * BLK), BF16),
            pltpu.VMEM((rows, WIDE), F32),
        ],
        compiler_params=pltpu.CompilerParams(vmem_limit_bytes=48 * 2**20),
        name="main",
    )(live, field, aplus, aminus, bplus, bminus, connectivity, blocks)
    rm = shift(mone, -1)
    rp = shift(pone, 1)
    rm3 = shift(jnp.concatenate([rm[9:18], own2, rp[9:18]]), -3)
    rp3 = shift(jnp.concatenate([rm[18:], own6, rp[18:]]), 3)
    rows = pad16(6 * OWN_ROWS)
    return pl.pallas_call(
        spread_kernel,
        out_shape=f(3, NODES),
        in_specs=[VMEM] * 6,
        out_specs=VMEM,
        scratch_shapes=[
            pltpu.VMEM((rows, LANES), BF16),
            pltpu.VMEM((WIDE, LANES), BF16),
            pltpu.VMEM((8, GHOST), F32),
            pltpu.VMEM((8, GHOST), F32),
            pltpu.VMEM((WIDE, 8 * GHOST), BF16),
            pltpu.VMEM((rows, 8 * GHOST), BF16),
        ],
        name="spread",
    )(own, rm, rp, rm3, rp3, send_nodes)


def solution(mesh):
    return jax.shard_map(
        body,
        mesh=mesh,
        in_specs=(P(None, "dom"), P(None, None, "dom"), P(None, "dom"), P(None, "dom"), P()),
        out_specs=P(None, "dom"),
        check_vma=False,
    )
```

```python
import jax
import jax.numpy as jnp
from jax import lax
from jax.experimental import pallas as pl
from jax.experimental.pallas import tpu as pltpu
from jax.sharding import PartitionSpec as P

F32 = jnp.float32
BF16 = jnp.bfloat16
LANES = 128
WIDE = 256
BLK = 512
ELEMS = 4096
NBLK = ELEMS // BLK
NODES = 5632
GHOST = 384
SLOTS = NODES + 8 * GHOST
OWN_ROWS = NODES // WIDE
ALL_ROWS = SLOTS // WIDE
TILES = BLK // LANES
VMEM = pl.BlockSpec(memory_space=pltpu.VMEM)
HBM = pl.BlockSpec(memory_space=pltpu.HBM)


def pad16(n):
    return -(-n // 16) * 16


def iota_rows(rows):
    return lax.broadcasted_iota(jnp.int32, (rows, LANES), 0)


def row_upper(rows):
    q = iota_rows(pad16(6 * rows))
    u = q
    for s in range(1, 6):
        u = jnp.where(q >= s * rows, q - s * rows, u)
    return jnp.where(q >= 6 * rows, -1, u)


def one_hot(const_ref, row):
    n = const_ref.shape[0]
    wide = jnp.broadcast_to(row, (16, LANES)).astype(BF16)
    out = []
    for g in range(n // 16):
        out.append(jnp.where(const_ref[pl.ds(16 * g, 16), :] == wide, jnp.ones((), BF16), jnp.zeros((), BF16)))
    return jnp.concatenate(out, axis=0)


def split(x):
    hi = x.astype(BF16).astype(F32)
    return hi, x - hi


def placed(const_ref, row, parts, rows):
    wide = jnp.broadcast_to(row, (16, LANES)).astype(BF16)
    vals = [jnp.broadcast_to(p, (16, LANES)).astype(BF16) for p in parts]
    sub = lax.broadcasted_iota(jnp.int32, (16, LANES), 0)
    zero = jnp.zeros((16, LANES), BF16)
    out = []
    for g in range(const_ref.shape[0] // 16):
        first, last = 16 * g // rows, (16 * g + 15) // rows
        value = vals[min(first, 5)]
        if last != first and last <= 5:
            cut = (first + 1) * rows - 16 * g
            value = jnp.where((sub < cut).astype(F32).astype(BF16) > 0, value, vals[last])
        out.append(jnp.where(const_ref[pl.ds(16 * g, 16), :] == wide, value, zero))
    return jnp.concatenate(out, axis=0)


def side():
    return lax.rem(lax.axis_index("dom"), 2)


def by_label(x):
    return jnp.where(side() == 1, pltpu.roll(x, 4, axis=0), x)


def pick_kernel(field_hbm, send_hbm, swap_ref, out_ref, field_ref, send_ref, sem):
    copies = [pltpu.make_async_copy(field_hbm, field_ref, sem.at[0]), pltpu.make_async_copy(send_hbm, send_ref, sem.at[1])]
    for copy in copies:
        copy.start()
    for copy in copies:
        copy.wait()
    place = {0: (swap_ref, 0), 4: (swap_ref, 9), 5: (swap_ref, 18), 6: (swap_ref, 27), 7: (swap_ref, 36),
             1: (out_ref, 0), 2: (out_ref, 9), 3: (out_ref, 18)}
    for j in range(3):
        index = by_label(send_ref[:, pl.ds(j * LANES, LANES)])
        upper, lower = index >> 7, index & 127
        total = [jnp.zeros((8, LANES), F32) for _ in range(3)]
        for h in range(NODES // LANES):
            hit = upper == h
            for c in range(3):
                row = jnp.broadcast_to(field_ref[pl.ds(c, 1), pl.ds(h * LANES, LANES)], (8, LANES))
                total[c] = jnp.where(hit, jnp.take_along_axis(row, lower, axis=1), total[c])
        for c in range(3):
            for m in range(8):
                ref, base = place[m]
                ref[pl.ds(base + c * 3 + j, 1), :] = total[c][m:m + 1, :]


def main_kernel(live_ref, field_hbm, near_ref, one_ref, two_ref, last_ref, conn_hbm, blocks_ref,
                own_ref, swap_ref, one_out_ref, two_out_ref,
                field_ref, conn_ref, early, stiff, sem, tf, table, upper_f, upper_b, lower_b, lo, up, hot, vals, force, put, total):
    n = live_ref[lax.axis_index("dom")]
    second = side() == 1
    field_copy = pltpu.make_async_copy(field_hbm, field_ref, early.at[0])
    conn_copy = pltpu.make_async_copy(conn_hbm, conn_ref, early.at[1])
    field_copy.start()
    conn_copy.start()

    def fetch(b):
        cols = pl.ds(pl.multiple_of(b * BLK, BLK), BLK)
        return pltpu.make_async_copy(blocks_ref.at[:, :, cols], stiff.at[b], sem.at[b])

    def start(b, _):
        fetch(b).start()
        return 0

    lax.fori_loop(0, n, start, 0)

    ru = row_upper(ALL_ROWS).astype(F32)
    upper_f[...] = ru
    upper_b[...] = ru.astype(BF16)
    lower_b[...] = iota_rows(WIDE).astype(F32).astype(BF16)

    tf[pl.ds(200, 8), :] = jnp.zeros((8, WIDE), F32)

    def fill(x, c, h):
        hi, low = split(x)
        for part, y in ((0, hi), (1, low)):
            tf[pl.ds((c * 2 + part) * ALL_ROWS + h // 2, 1), pl.ds((h % 2) * LANES, LANES)] = y

    field_copy.wait()
    for h in range(NODES // LANES):
        x = field_ref[:, pl.ds(h * LANES, LANES)]
        for c in range(3):
            fill(x[c:c + 1, :], c, h)
    source = {0: (one_ref, 9), 1: (one_ref, 0), 2: (two_ref, 9), 3: (two_ref, 0),
              4: (near_ref, 0), 5: (last_ref, 9), 6: (last_ref, 0), 7: (last_ref, 18)}
    ghost = [source[m][0][pl.ds(source[m][1], 9), :] for m in range(8)]
    for k in range(8):
        bundle = jnp.where(second, ghost[k ^ 4], ghost[k])
        for c in range(3):
            for j in range(3):
                q = c * 3 + j
                fill(bundle[q:q + 1, :], c, NODES // LANES + 3 * k + j)
    table[...] = tf[...].astype(BF16)
    total[...] = jnp.zeros_like(total)
    conn_copy.wait()

    def step(b, _):
        index = conn_ref[:, pl.ds(pl.multiple_of(b * BLK, BLK), BLK)]
        lo[...] = (index & (WIDE - 1)).astype(F32)
        up[...] = (index >> 8).astype(F32)
        for a in range(10):
            for t2 in range(TILES // 2):
                at = (a * TILES + 2 * t2) * LANES
                for s in range(2):
                    row = lo[pl.ds(a, 1), pl.ds((2 * t2 + s) * LANES, LANES)]
                    hot[:, pl.ds(at + s * LANES, LANES)] = one_hot(lower_b, row)
                got = jnp.dot(table[...], hot[:, pl.ds(at, WIDE)], preferred_element_type=F32)
                for s in range(2):
                    row = jnp.broadcast_to(up[pl.ds(a, 1), pl.ds((2 * t2 + s) * LANES, LANES)], (8, LANES))
                    sums = [None, None, None]
                    for g in range(26):
                        hit = jnp.where(upper_f[pl.ds(8 * g, 8), :] == row,
                                        got[8 * g:8 * g + 8, s * LANES:(s + 1) * LANES], 0.0)
                        if g == 8:
                            head = iota_rows(8) < 4
                            sums[0] = sums[0] + jnp.where(head, hit, 0.0)
                            sums[1] = jnp.where(head, 0.0, hit)
                        else:
                            c = 0 if g < 8 else (1 if g < 17 else 2)
                            sums[c] = hit if sums[c] is None else sums[c] + hit
                    for c in range(3):
                        vals[pl.ds(c * 10 + a, 1), pl.ds((2 * t2 + s) * LANES, LANES)] = jnp.sum(sums[c], axis=0, keepdims=True)
        fetch(b).wait()
        for t in range(TILES):
            v = vals[:, pl.ds(t * LANES, LANES)]
            for i in range(30):
                k = stiff[b, i, :, pl.ds(t * LANES, LANES)].astype(F32)
                force[pl.ds(i, 1), pl.ds(t * LANES, LANES)] = jnp.sum(k * v, axis=0, keepdims=True)
        for a in range(10):
            for t in range(TILES):
                parts = []
                for c in range(3):
                    parts.extend(split(force[pl.ds(c * 10 + a, 1), pl.ds(t * LANES, LANES)]))
                row = up[pl.ds(a, 1), pl.ds(t * LANES, LANES)]
                put[:, pl.ds((a * TILES + t) * LANES, LANES)] = placed(upper_b, row, parts, ALL_ROWS)
        total[...] += lax.dot_general(put[...], hot[...], (((1,), (1,)), ((), ())), preferred_element_type=F32)
        return 0

    lax.fori_loop(0, n, step, 0)

    for c in range(3):
        base = 2 * c * ALL_ROWS
        own_ref[pl.ds(c * OWN_ROWS, OWN_ROWS), :] = total[pl.ds(base, OWN_ROWS), :] + total[pl.ds(base + ALL_ROWS, OWN_ROWS), :]
    target = {6: (swap_ref, 0), 5: (swap_ref, 9), 7: (swap_ref, 18), 4: (swap_ref, 27),
              1: (one_out_ref, 0), 0: (one_out_ref, 9), 3: (two_out_ref, 0), 2: (two_out_ref, 9)}

    def partial(k, c, j):
        h = NODES // LANES + 3 * k + j
        at = 2 * c * ALL_ROWS + h // 2
        cols = pl.ds((h % 2) * LANES, LANES)
        return total[pl.ds(at, 1), cols] + total[pl.ds(at + ALL_ROWS, 1), cols]

    for m in range(4):
        for c in range(3):
            for j in range(3):
                low, high = partial(m, c, j), partial(m + 4, c, j)
                for label, x in ((m, jnp.where(second, high, low)), (m + 4, jnp.where(second, low, high))):
                    ref, base = target[label]
                    ref[pl.ds(base + c * 3 + j, 1), :] = x


def spread_kernel(own_ref, swap_ref, one_ref, two_ref, last_ref, send_ref, out_ref, upper_b, lower_b, lo, up, hot, put):
    upper_b[...] = row_upper(OWN_ROWS).astype(F32).astype(BF16)
    lower_b[...] = iota_rows(WIDE).astype(F32).astype(BF16)
    index = by_label(send_ref[...])
    lo[...] = (index & (WIDE - 1)).astype(F32)
    up[...] = (index >> 8).astype(F32)
    source = {0: (swap_ref, 27), 1: (one_ref, 0), 2: (one_ref, 18), 3: (two_ref, 0),
              4: (last_ref, 0), 5: (last_ref, 9), 6: (last_ref, 18), 7: (last_ref, 27)}
    for k in range(8):
        ref, base = source[k]
        for j in range(3):
            at = pl.ds((3 * k + j) * LANES, LANES)
            cols = pl.ds(j * LANES, LANES)
            hot[:, at] = one_hot(lower_b, lo[pl.ds(k, 1), cols])
            parts = []
            for c in range(3):
                parts.extend(split(ref[pl.ds(base + c * 3 + j, 1), :]))
            put[:, at] = placed(upper_b, up[pl.ds(k, 1), cols], parts, OWN_ROWS)
    total = lax.dot_general(put[...], hot[...], (((1,), (1,)), ((), ())), preferred_element_type=F32)
    for c in range(3):
        for u in range(OWN_ROWS):
            q = 2 * c * OWN_ROWS + u
            out_ref[pl.ds(c, 1), pl.ds(u * WIDE, WIDE)] = (
                total[q:q + 1, :] + total[q + OWN_ROWS:q + OWN_ROWS + 1, :] + own_ref[pl.ds(c * OWN_ROWS + u, 1), :]
            )


def across(x):
    return lax.ppermute(x, "dom", [(i, i ^ 1) for i in range(lax.axis_size("dom"))])


def along(x, o):
    n = lax.axis_size("dom")
    return lax.ppermute(x, "dom", [(i, (i + (2 * o if i % 2 == 0 else -2 * o)) % n) for i in range(n)])


def in_hbm(x):
    return pltpu.with_memory_space_constraint(x, pltpu.HBM)


def params(kib):
    return pltpu.CompilerParams(vmem_limit_bytes=kib * 1024)


def body(field, blocks, connectivity, send_nodes, live_blocks):
    f = lambda *s: jax.ShapeDtypeStruct(s, F32)
    swap, out = pl.pallas_call(
        pick_kernel, out_shape=(f(45, LANES), f(27, LANES)), in_specs=[HBM] * 2, out_specs=(VMEM,) * 2,
        scratch_shapes=[pltpu.VMEM((3, NODES), F32), pltpu.VMEM((8, GHOST), jnp.int32), pltpu.SemaphoreType.DMA((2,))],
        compiler_params=params(1024), name="pick",
    )(in_hbm(field), in_hbm(send_nodes))
    near = across(swap)
    one = along(jnp.concatenate([out[:9], near[9:18], out[9:18], near[18:27]]), 1)
    two = along(jnp.concatenate([out[18:], near[27:]]), 2)
    last = across(jnp.concatenate([one[18:], two[18:]]))
    rows = pad16(6 * ALL_ROWS)
    own, swap, one_out, two_out = pl.pallas_call(
        main_kernel,
        out_shape=(f(3 * OWN_ROWS, WIDE), f(36, LANES), f(18, LANES), f(18, LANES)),
        in_specs=[pl.BlockSpec(memory_space=pltpu.SMEM), HBM] + [VMEM] * 4 + [HBM] * 2,
        out_specs=(VMEM,) * 4,
        scratch_shapes=[
            pltpu.VMEM((3, NODES), F32),
            pltpu.VMEM((10, ELEMS), jnp.int32),
            pltpu.SemaphoreType.DMA((2,)),
            pltpu.VMEM((NBLK, 30, 30, BLK), BF16),
            pltpu.SemaphoreType.DMA((NBLK,)),
            pltpu.VMEM((rows, WIDE), F32),
            pltpu.VMEM((rows, WIDE), BF16),
            pltpu.VMEM((rows, LANES), F32),
            pltpu.VMEM((rows, LANES), BF16),
            pltpu.VMEM((WIDE, LANES), BF16),
            pltpu.VMEM((10, BLK), F32),
            pltpu.VMEM((10, BLK), F32),
            pltpu.VMEM((WIDE, 10 * BLK), BF16),
            pltpu.VMEM((30, BLK), F32),
            pltpu.VMEM((30, BLK), F32),
            pltpu.VMEM((rows, 10 * BLK), BF16),
            pltpu.VMEM((rows, WIDE), F32),
        ],
        compiler_params=params(32768),
        name="main",
    )(in_hbm(live_blocks), in_hbm(field), near, one, two, last, in_hbm(connectivity), in_hbm(blocks))
    swapped = across(swap)
    one_in = along(jnp.concatenate([one_out, swapped[:18]]), -1)
    two_in = along(jnp.concatenate([two_out, swapped[18:27]]), -2)
    back = across(jnp.concatenate([one_in[9:18], one_in[27:], two_in[9:]]))
    rows = pad16(6 * OWN_ROWS)
    return pl.pallas_call(
        spread_kernel,
        out_shape=f(3, NODES),
        in_specs=[VMEM] * 6,
        out_specs=VMEM,
        scratch_shapes=[
            pltpu.VMEM((rows, LANES), BF16),
            pltpu.VMEM((WIDE, LANES), BF16),
            pltpu.VMEM((8, GHOST), F32),
            pltpu.VMEM((8, GHOST), F32),
            pltpu.VMEM((WIDE, 8 * GHOST), BF16),
            pltpu.VMEM((rows, 8 * GHOST), BF16),
        ],
        compiler_params=params(8192),
        name="spread",
    )(own, swapped, one_in, two_in, back, send_nodes)


def solution(mesh):
    return jax.shard_map(
        body,
        mesh=mesh,
        in_specs=(P(None, "dom"), P(None, None, "dom"), P(None, "dom"), P(None, "dom"), P()),
        out_specs=P(None, "dom"),
        check_vma=False,
    )
```

```python
import jax
import jax.numpy as jnp
from jax import lax
from jax.experimental import pallas as pl
from jax.experimental.pallas import tpu as pltpu
from jax.sharding import PartitionSpec as P

F32 = jnp.float32
BF16 = jnp.bfloat16
LANES = 128
WIDE = 256
BLK = 512
ELEMS = 4096
NBLK = ELEMS // BLK
NODES = 5632
GHOST = 384
SLOTS = NODES + 8 * GHOST
OWN_ROWS = NODES // WIDE
ALL_ROWS = SLOTS // WIDE
TILES = BLK // LANES
VMEM = pl.BlockSpec(memory_space=pltpu.VMEM)
HBM = pl.BlockSpec(memory_space=pltpu.HBM)


def pad16(n):
    return -(-n // 16) * 16


def iota_rows(rows):
    return lax.broadcasted_iota(jnp.int32, (rows, LANES), 0)


def row_upper(rows, first, count):
    q = iota_rows(count) + first
    u = q
    for s in range(1, 6):
        u = jnp.where(q >= s * rows, q - s * rows, u)
    return jnp.where(q >= 6 * rows, -1, u).astype(F32)


def lower_parts():
    return [(iota_rows(16) + 16 * g).astype(F32).astype(BF16) for g in range(WIDE // 16)]


def upper_parts(rows):
    return [row_upper(rows, 16 * g, 16).astype(BF16) for g in range(pad16(6 * rows) // 16)]


def wide(row):
    return jnp.broadcast_to(row, (16, LANES)).astype(BF16)


def one_hot(parts, row):
    here, one, zero = wide(row), jnp.ones((16, LANES), BF16), jnp.zeros((16, LANES), BF16)
    return jnp.concatenate([jnp.where(part == here, one, zero) for part in parts], axis=0)


def split(x):
    hi = x.astype(BF16).astype(F32)
    return hi, x - hi


def placed(uppers, row, values, rows):
    here, zero = wide(row), jnp.zeros((16, LANES), BF16)
    values = [wide(v) for v in values]
    out = []
    for g, upper in enumerate(uppers):
        first, last = 16 * g // rows, (16 * g + 15) // rows
        value = values[min(first, 5)]
        if last != first and last <= 5:
            cut = (first + 1) * rows - 16 * g
            head = iota_rows(16).astype(F32).astype(BF16) < jnp.full((16, LANES), cut, BF16)
            value = jnp.where(head, value, values[last])
        out.append(jnp.where(upper == here, value, zero))
    return jnp.concatenate(out, axis=0)


def side():
    return lax.rem(lax.axis_index("dom"), 2)


def by_label(x):
    return jnp.where(side() == 1, pltpu.roll(x, 4, axis=0), x)


def pick_kernel(field_hbm, send_hbm, swap_ref, out_ref, field_ref, send_ref, sem):
    copies = [pltpu.make_async_copy(field_hbm, field_ref, sem.at[0]), pltpu.make_async_copy(send_hbm, send_ref, sem.at[1])]
    for copy in copies:
        copy.start()
    for copy in copies:
        copy.wait()
    place = {0: (swap_ref, 0), 4: (swap_ref, 9), 5: (swap_ref, 18), 6: (swap_ref, 27), 7: (swap_ref, 36),
             1: (out_ref, 0), 2: (out_ref, 9), 3: (out_ref, 18)}
    for j in range(3):
        index = by_label(send_ref[:, pl.ds(j * LANES, LANES)])
        upper, lower = index >> 7, index & 127
        total = [jnp.zeros((8, LANES), F32) for _ in range(3)]
        for h in range(NODES // LANES):
            hit = upper == h
            for c in range(3):
                row = jnp.broadcast_to(field_ref[pl.ds(c, 1), pl.ds(h * LANES, LANES)], (8, LANES))
                total[c] = jnp.where(hit, jnp.take_along_axis(row, lower, axis=1), total[c])
        for c in range(3):
            for m in range(8):
                ref, base = place[m]
                ref[pl.ds(base + c * 3 + j, 1), :] = total[c][m:m + 1, :]


def main_kernel(live_ref, field_hbm, near_ref, one_ref, two_ref, last_ref, conn_hbm, blocks_ref,
                own_ref, swap_ref, one_out_ref, two_out_ref,
                field_ref, conn_ref, early, stiff, sem, tf, lo, up, vals, high, low, total):
    n = live_ref[lax.axis_index("dom")]
    second = side() == 1
    field_copy = pltpu.make_async_copy(field_hbm, field_ref, early.at[0])
    conn_copy = pltpu.make_async_copy(conn_hbm, conn_ref, early.at[1])
    field_copy.start()
    conn_copy.start()

    def fetch(b):
        cols = pl.ds(pl.multiple_of(b * BLK, BLK), BLK)
        return pltpu.make_async_copy(blocks_ref.at[:, :, cols], stiff.at[b], sem.at[b])

    def start(b, _):
        fetch(b).start()
        return 0

    lax.fori_loop(0, n, start, 0)

    tf[pl.ds(200, 8), :] = jnp.zeros((8, WIDE), F32)

    def fill(x, c, h):
        hi, low = split(x)
        for part, y in ((0, hi), (1, low)):
            tf[pl.ds((c * 2 + part) * ALL_ROWS + h // 2, 1), pl.ds((h % 2) * LANES, LANES)] = y

    field_copy.wait()
    for h in range(NODES // LANES):
        x = field_ref[:, pl.ds(h * LANES, LANES)]
        for c in range(3):
            fill(x[c:c + 1, :], c, h)
    source = {0: (one_ref, 9), 1: (one_ref, 0), 2: (two_ref, 9), 3: (two_ref, 0),
              4: (near_ref, 0), 5: (last_ref, 9), 6: (last_ref, 0), 7: (last_ref, 18)}
    ghost = [source[m][0][pl.ds(source[m][1], 9), :] for m in range(8)]
    for k in range(8):
        bundle = jnp.where(second, ghost[k ^ 4], ghost[k])
        for c in range(3):
            for j in range(3):
                q = c * 3 + j
                fill(bundle[q:q + 1, :], c, NODES // LANES + 3 * k + j)
    table = tf[...].astype(BF16)
    lowers, uppers = lower_parts(), upper_parts(ALL_ROWS)
    per = 2 * ALL_ROWS
    even = [row_upper(ALL_ROWS, 8 * g, 8) for g in range(9)]
    odd = [row_upper(ALL_ROWS, 8 * g, 8) for g in range(8, 17)]
    head = iota_rows(8) < per % 8
    even[8] = jnp.where(head, even[8], -1.0)
    odd[0] = jnp.where(head, -1.0, odd[0])
    total[...] = jnp.zeros_like(total)
    conn_copy.wait()

    def step(b, _):
        index = conn_ref[:, pl.ds(pl.multiple_of(b * BLK, BLK), BLK)]
        lo[...] = (index & (WIDE - 1)).astype(F32)
        up[...] = (index >> 8).astype(F32)
        for a in range(10):
            for t2 in range(TILES // 2):
                cols = [pl.ds((2 * t2 + s) * LANES, LANES) for s in range(2)]
                hot = jnp.concatenate([one_hot(lowers, lo[pl.ds(a, 1), c]) for c in cols], axis=1)
                got = jnp.dot(table, hot, preferred_element_type=F32)
                for s in range(2):
                    here = jnp.broadcast_to(up[pl.ds(a, 1), cols[s]], (8, LANES))
                    sums = [jnp.zeros((8, LANES), F32)] * 3
                    for g in range(9):
                        hit = even[g] == here
                        for c in (0, 2):
                            q = 8 * g + c * per
                            sums[c] = jnp.where(hit, got[q:q + 8, s * LANES:(s + 1) * LANES], sums[c])
                        q = 64 + 8 * g
                        sums[1] = jnp.where(odd[g] == here, got[q:q + 8, s * LANES:(s + 1) * LANES], sums[1])
                    for c in range(3):
                        vals[pl.ds(c * 10 + a, 1), cols[s]] = jnp.sum(sums[c], axis=0, keepdims=True)
        fetch(b).wait()
        for t in range(TILES):
            cols = pl.ds(t * LANES, LANES)
            v = vals[:, cols]
            for i in range(30):
                k = stiff[b, i, :, cols].astype(F32)
                high[pl.ds(i, 1), cols] = jnp.sum(k * v, axis=0, keepdims=True)
        high[...], low[...] = split(high[...])
        acc = None
        for a in range(10):
            for t2 in range(TILES // 2):
                hot, put = [], []
                for s in range(2):
                    cols = pl.ds((2 * t2 + s) * LANES, LANES)
                    hot.append(one_hot(lowers, lo[pl.ds(a, 1), cols]))
                    values = [ref[pl.ds(c * 10 + a, 1), cols] for c in range(3) for ref in (high, low)]
                    put.append(placed(uppers, up[pl.ds(a, 1), cols], values, ALL_ROWS))
                part = lax.dot_general(jnp.concatenate(put, axis=1), jnp.concatenate(hot, axis=1), (((1,), (1,)), ((), ())),
                                       preferred_element_type=F32)
                acc = part if acc is None else acc + part
        total[...] += acc
        return 0

    lax.fori_loop(0, n, step, 0)

    for c in range(3):
        base = 2 * c * ALL_ROWS
        own_ref[pl.ds(c * OWN_ROWS, OWN_ROWS), :] = total[pl.ds(base, OWN_ROWS), :] + total[pl.ds(base + ALL_ROWS, OWN_ROWS), :]
    target = {6: (swap_ref, 0), 5: (swap_ref, 9), 7: (swap_ref, 18), 4: (swap_ref, 27),
              1: (one_out_ref, 0), 0: (one_out_ref, 9), 3: (two_out_ref, 0), 2: (two_out_ref, 9)}

    def partial(k, c, j):
        h = NODES // LANES + 3 * k + j
        at = 2 * c * ALL_ROWS + h // 2
        cols = pl.ds((h % 2) * LANES, LANES)
        return total[pl.ds(at, 1), cols] + total[pl.ds(at + ALL_ROWS, 1), cols]

    for m in range(4):
        for c in range(3):
            for j in range(3):
                low, high = partial(m, c, j), partial(m + 4, c, j)
                for label, x in ((m, jnp.where(second, high, low)), (m + 4, jnp.where(second, low, high))):
                    ref, base = target[label]
                    ref[pl.ds(base + c * 3 + j, 1), :] = x


def spread_kernel(own_ref, swap_ref, one_ref, two_ref, last_ref, send_ref, out_ref, lo, up):
    lowers, uppers = lower_parts(), upper_parts(OWN_ROWS)
    index = by_label(send_ref[...])
    lo[...] = (index & (WIDE - 1)).astype(F32)
    up[...] = (index >> 8).astype(F32)
    source = {0: (swap_ref, 27), 1: (one_ref, 0), 2: (one_ref, 18), 3: (two_ref, 0),
              4: (last_ref, 0), 5: (last_ref, 9), 6: (last_ref, 18), 7: (last_ref, 27)}
    hot, put = [], []
    for m in range(8):
        ref, base = source[m]
        for j in range(3):
            cols = pl.ds(j * LANES, LANES)
            hot.append(one_hot(lowers, lo[pl.ds(m, 1), cols]))
            values = [x for c in range(3) for x in split(ref[pl.ds(base + c * 3 + j, 1), :])]
            put.append(placed(uppers, up[pl.ds(m, 1), cols], values, OWN_ROWS))
    total = None
    for g in range(0, 24, 2):
        part = lax.dot_general(jnp.concatenate(put[g:g + 2], axis=1), jnp.concatenate(hot[g:g + 2], axis=1),
                               (((1,), (1,)), ((), ())), preferred_element_type=F32)
        total = part if total is None else total + part
    for c in range(3):
        for u in range(OWN_ROWS):
            q = 2 * c * OWN_ROWS + u
            out_ref[pl.ds(c, 1), pl.ds(u * WIDE, WIDE)] = (
                total[q:q + 1, :] + total[q + OWN_ROWS:q + OWN_ROWS + 1, :] + own_ref[pl.ds(c * OWN_ROWS + u, 1), :]
            )


def across(x):
    return lax.ppermute(x, "dom", [(i, i ^ 1) for i in range(lax.axis_size("dom"))])


def along(x, o):
    n = lax.axis_size("dom")
    route = {i: i + (2 * o if i % 2 == 0 else -2 * o) for i in range(n)}
    spare = sorted(set(range(n)) - set(route.values()))
    for i in range(n):
        if route[i] not in range(n):
            route[i] = min(spare, key=lambda j: (abs(j - i), j))
            spare.remove(route[i])
    return lax.ppermute(x, "dom", list(route.items()))


def in_hbm(x):
    return pltpu.with_memory_space_constraint(x, pltpu.HBM)


def params(kib):
    return pltpu.CompilerParams(vmem_limit_bytes=kib * 1024)


def body(field, blocks, connectivity, send_nodes, live_blocks):
    f = lambda *s: jax.ShapeDtypeStruct(s, F32)
    swap, out = pl.pallas_call(
        pick_kernel, out_shape=(f(45, LANES), f(27, LANES)), in_specs=[HBM] * 2, out_specs=(VMEM,) * 2,
        scratch_shapes=[pltpu.VMEM((3, NODES), F32), pltpu.VMEM((8, GHOST), jnp.int32), pltpu.SemaphoreType.DMA((2,))],
        compiler_params=params(1024), name="pick",
    )(in_hbm(field), in_hbm(send_nodes))
    near = across(swap)
    one = along(jnp.concatenate([out[:9], near[9:18], out[9:18], near[18:27]]), 1)
    two = along(jnp.concatenate([out[18:], near[27:]]), 2)
    last = across(jnp.concatenate([one[18:], two[18:]]))
    rows = pad16(6 * ALL_ROWS)
    own, swap, one_out, two_out = pl.pallas_call(
        main_kernel,
        out_shape=(f(3 * OWN_ROWS, WIDE), f(36, LANES), f(18, LANES), f(18, LANES)),
        in_specs=[pl.BlockSpec(memory_space=pltpu.SMEM), HBM] + [VMEM] * 4 + [HBM] * 2,
        out_specs=(VMEM,) * 4,
        scratch_shapes=[
            pltpu.VMEM((3, NODES), F32),
            pltpu.VMEM((10, ELEMS), jnp.int32),
            pltpu.SemaphoreType.DMA((2,)),
            pltpu.VMEM((NBLK, 30, 30, BLK), BF16),
            pltpu.SemaphoreType.DMA((NBLK,)),
            pltpu.VMEM((rows, WIDE), F32),
            pltpu.VMEM((10, BLK), F32),
            pltpu.VMEM((10, BLK), F32),
            pltpu.VMEM((30, BLK), F32),
            pltpu.VMEM((30, BLK), F32),
            pltpu.VMEM((30, BLK), F32),
            pltpu.VMEM((rows, WIDE), F32),
        ],
        compiler_params=params(32768),
        name="main",
    )(in_hbm(live_blocks), in_hbm(field), near, one, two, last, in_hbm(connectivity), in_hbm(blocks))
    swapped = across(swap)
    one_in = along(jnp.concatenate([one_out, swapped[:18]]), -1)
    two_in = along(jnp.concatenate([two_out, swapped[18:27]]), -2)
    back = across(jnp.concatenate([one_in[9:18], one_in[27:], two_in[9:]]))
    return pl.pallas_call(
        spread_kernel,
        out_shape=f(3, NODES),
        in_specs=[VMEM] * 6,
        out_specs=VMEM,
        scratch_shapes=[
            pltpu.VMEM((8, GHOST), F32),
            pltpu.VMEM((8, GHOST), F32),
        ],
        compiler_params=params(8192),
        name="spread",
    )(own, swapped, one_in, two_in, back, send_nodes)


def solution(mesh):
    return jax.shard_map(
        body,
        mesh=mesh,
        in_specs=(P(None, "dom"), P(None, None, "dom"), P(None, "dom"), P(None, "dom"), P()),
        out_specs=P(None, "dom"),
        check_vma=False,
    )
```

```python
import jax
import jax.numpy as jnp
from jax import lax
from jax.experimental import pallas as pl
from jax.experimental.pallas import tpu as pltpu
from jax.sharding import PartitionSpec as P


F32 = jnp.float32
BF16 = jnp.bfloat16
LANES = 128
WIDE = 256
BLK = 512
ELEMS = 4096
NBLK = ELEMS // BLK
NODES = 5632
GHOST = 384
SLOTS = NODES + 8 * GHOST
OWN_ROWS = NODES // WIDE
ALL_ROWS = SLOTS // WIDE
GHOST_ROWS = ALL_ROWS - OWN_ROWS
TILES = BLK // LANES
VMEM = pl.BlockSpec(memory_space=pltpu.VMEM)
HBM = pl.BlockSpec(memory_space=pltpu.HBM)


def pad16(n):
    return -(-n // 16) * 16


def iota_rows(rows):
    return lax.broadcasted_iota(jnp.int32, (rows, LANES), 0)


def row_upper(rows, first, count):
    q = iota_rows(count) + first
    u = q
    for s in range(1, 6):
        u = jnp.where(q >= s * rows, q - s * rows, u)
    return jnp.where(q >= 6 * rows, -1, u).astype(F32)


def table_rows(rows):
    return pad16(6 * rows)


def select_parts(rows):
    per = 2 * rows
    out, seen = [], {}
    for g in range(-(-3 * per // 8)):
        for c in sorted({min(8 * g // per, 2), min((8 * g + 7) // per, 2)}):
            key = (max(8 * g, c * per) - c * per, min(8 * g + 8, c * per + per) - c * per, (c * per) % 8)
            if key not in seen:
                upper = row_upper(rows, 8 * g, 8)
                q = iota_rows(8) + 8 * g
                if 8 * g < c * per or 8 * g + 8 > c * per + per:
                    upper = jnp.where((q >= c * per) & (q < c * per + per), upper, -1.0)
                seen[key] = upper
            out.append((g, c, key))
    return out, seen


def select_sums(parts, row, got, lanes):
    order, uppers = parts
    here = jnp.broadcast_to(row, (8, LANES))
    hits, sums = {}, [jnp.zeros((8, LANES), F32)] * 3
    for g, c, key in order:
        if key not in hits:
            hits[key] = uppers[key] == here
        sums[c] = jnp.where(hits[key], got[8 * g:8 * g + 8, lanes:lanes + LANES], sums[c])
    return sums


def fill(tf, rows, x, c, h):
    hi, low = split(x)
    for part, y in ((0, hi), (1, low)):
        tf[pl.ds((c * 2 + part) * rows + h // 2, 1), pl.ds((h % 2) * LANES, LANES)] = y


def lower_parts():
    return [(iota_rows(16) + 16 * g).astype(F32).astype(BF16) for g in range(WIDE // 16)]


def upper_parts(rows):
    return [row_upper(rows, 16 * g, 16).astype(BF16) for g in range(pad16(6 * rows) // 16)]


def wide(row):
    return jnp.broadcast_to(row, (16, LANES)).astype(BF16)


def one_hot(parts, row):
    here, one, zero = wide(row), jnp.ones((16, LANES), BF16), jnp.zeros((16, LANES), BF16)
    return jnp.concatenate([jnp.where(part == here, one, zero) for part in parts], axis=0)


def split(x):
    hi = x.astype(BF16).astype(F32)
    return hi, x - hi


def placed(uppers, row, values, rows):
    here, zero = wide(row), jnp.zeros((16, LANES), BF16)
    values = [wide(v) for v in values]
    out = []
    for g, upper in enumerate(uppers):
        first, last = 16 * g // rows, (16 * g + 15) // rows
        value = values[min(first, 5)]
        if last != first and last <= 5:
            cut = (first + 1) * rows - 16 * g
            head = iota_rows(16).astype(F32).astype(BF16) < jnp.full((16, LANES), cut, BF16)
            value = jnp.where(head, value, values[last])
        out.append(jnp.where(upper == here, value, zero))
    return jnp.concatenate(out, axis=0)


def side():
    return lax.rem(lax.axis_index("dom"), 2)


def by_label(x):
    return jnp.where(side() == 1, pltpu.roll(x, 4, axis=0), x)


def pick_kernel(field_hbm, send_hbm, conn_hbm, swap_ref, out_ref, field_ref, conn_ref, send_ref, sem):
    copies = [pltpu.make_async_copy(field_hbm, field_ref, sem.at[0]), pltpu.make_async_copy(send_hbm, send_ref, sem.at[1]),
              pltpu.make_async_copy(conn_hbm, conn_ref, sem.at[2])]
    for copy in copies:
        copy.start()
    copies[0].wait()
    copies[1].wait()
    place = {0: (swap_ref, 0), 4: (swap_ref, 9), 5: (swap_ref, 18), 6: (swap_ref, 27), 7: (swap_ref, 36),
             1: (out_ref, 0), 2: (out_ref, 9), 3: (out_ref, 18)}
    for j in range(3):
        index = by_label(send_ref[:, pl.ds(j * LANES, LANES)])
        upper, lower = index >> 7, index & 127
        total = [jnp.zeros((8, LANES), F32) for _ in range(3)]
        for h in range(NODES // LANES):
            hit = upper == h
            for c in range(3):
                row = jnp.broadcast_to(field_ref[pl.ds(c, 1), pl.ds(h * LANES, LANES)], (8, LANES))
                total[c] = jnp.where(hit, jnp.take_along_axis(row, lower, axis=1), total[c])
        for c in range(3):
            for m in range(8):
                ref, base = place[m]
                ref[pl.ds(base + c * 3 + j, 1), :] = total[c][m:m + 1, :]
    copies[2].wait()


def prep_kernel(live_ref, field_ref, conn_ref, after_ref, blocks_hbm, stiff_ref, sums_ref, lo_ref, up_ref, sem, tf):
    del after_ref
    n = live_ref[lax.axis_index("dom")]

    def fetch(b):
        return pltpu.make_async_copy(blocks_hbm.at[:, :, pl.ds(pl.multiple_of(b * BLK, BLK), BLK)], stiff_ref.at[b], sem.at[b])

    def start(b, _):
        fetch(b).start()
        return 0

    def wait(b, _):
        fetch(b).wait()
        return 0

    lax.fori_loop(0, n, start, 0)
    used = 6 * OWN_ROWS
    tf[pl.ds(used // 8 * 8, tf.shape[0] - used // 8 * 8), :] = jnp.zeros((tf.shape[0] - used // 8 * 8, WIDE), F32)
    for h in range(NODES // LANES):
        x = field_ref[:, pl.ds(h * LANES, LANES)]
        for c in range(3):
            fill(tf, OWN_ROWS, x[c:c + 1, :], c, h)
    table = tf[...].astype(BF16)
    lowers, parts = lower_parts(), select_parts(OWN_ROWS)

    def step(b, _):
        block = pl.ds(pl.multiple_of(b * BLK, BLK), BLK)
        index = conn_ref[:, block]
        lo_ref[b] = (index & (WIDE - 1)).astype(F32)
        up_ref[b] = (index >> 8).astype(F32)
        for a in range(10):
            for t2 in range(TILES // 2):
                cols = [pl.ds((2 * t2 + s) * LANES, LANES) for s in range(2)]
                hot = jnp.concatenate([one_hot(lowers, lo_ref[b, pl.ds(a, 1), c]) for c in cols], axis=1)
                got = jnp.dot(table, hot, preferred_element_type=F32)
                for s in range(2):
                    sums = select_sums(parts, up_ref[b, pl.ds(a, 1), cols[s]], got, s * LANES)
                    for c in range(3):
                        sums_ref[b, (a * TILES + 2 * t2 + s) * 3 + c] = sums[c]
        return 0

    lax.fori_loop(0, n, step, 0)
    lax.fori_loop(0, n, wait, 0)


def main_kernel(live_ref, near_ref, one_ref, two_ref, last_ref, stiff_ref, sums_ref, lo_ref, up_ref,
                own_ref, swap_ref, one_out_ref, two_out_ref, tf, vals, high, low, total):
    n = live_ref[lax.axis_index("dom")]
    second = side() == 1

    used = 6 * GHOST_ROWS
    tf[pl.ds(used, tf.shape[0] - used), :] = jnp.zeros((tf.shape[0] - used, WIDE), F32)
    source = {0: (one_ref, 9), 1: (one_ref, 0), 2: (two_ref, 9), 3: (two_ref, 0),
              4: (near_ref, 0), 5: (last_ref, 9), 6: (last_ref, 0), 7: (last_ref, 18)}
    ghost = [source[m][0][pl.ds(source[m][1], 9), :] for m in range(8)]
    for k in range(8):
        bundle = jnp.where(second, ghost[k ^ 4], ghost[k])
        for c in range(3):
            for j in range(3):
                q = c * 3 + j
                fill(tf, GHOST_ROWS, bundle[q:q + 1, :], c, 3 * k + j)
    table = tf[...].astype(BF16)
    total[...] = jnp.zeros_like(total)
    lowers, uppers, parts = lower_parts(), upper_parts(ALL_ROWS), select_parts(GHOST_ROWS)

    def step(b, _):
        hots = []
        for a in range(10):
            for t2 in range(TILES // 2):
                cols = [pl.ds((2 * t2 + s) * LANES, LANES) for s in range(2)]
                hot = jnp.concatenate([one_hot(lowers, lo_ref[b, pl.ds(a, 1), c]) for c in cols], axis=1)
                hots.append(hot)
                got = jnp.dot(table, hot, preferred_element_type=F32)
                for s in range(2):
                    sums = select_sums(parts, up_ref[b, pl.ds(a, 1), cols[s]] - OWN_ROWS, got, s * LANES)
                    for c in range(3):
                        sums[c] = sums[c] + sums_ref[b, (a * TILES + 2 * t2 + s) * 3 + c]
                        vals[pl.ds(c * 10 + a, 1), cols[s]] = jnp.sum(sums[c], axis=0, keepdims=True)
        for t in range(TILES):
            cols = pl.ds(t * LANES, LANES)
            v = vals[:, cols]
            for i in range(30):
                k = stiff_ref[b, i, :, cols].astype(F32)
                high[pl.ds(i, 1), cols] = jnp.sum(k * v, axis=0, keepdims=True)
        high[...], low[...] = split(high[...])
        acc = None
        for a in range(10):
            for t2 in range(TILES // 2):
                put = []
                for s in range(2):
                    cols = pl.ds((2 * t2 + s) * LANES, LANES)
                    values = [ref[pl.ds(c * 10 + a, 1), cols] for c in range(3) for ref in (high, low)]
                    put.append(placed(uppers, up_ref[b, pl.ds(a, 1), cols], values, ALL_ROWS))
                part = lax.dot_general(jnp.concatenate(put, axis=1), hots[a * (TILES // 2) + t2], (((1,), (1,)), ((), ())),
                                       preferred_element_type=F32)
                acc = part if acc is None else acc + part
        total[...] += acc
        return 0

    lax.fori_loop(0, n, step, 0)

    for c in range(3):
        base = 2 * c * ALL_ROWS
        own_ref[pl.ds(c * OWN_ROWS, OWN_ROWS), :] = total[pl.ds(base, OWN_ROWS), :] + total[pl.ds(base + ALL_ROWS, OWN_ROWS), :]
    target = {6: (swap_ref, 0), 5: (swap_ref, 9), 7: (swap_ref, 18), 4: (swap_ref, 27),
              1: (one_out_ref, 0), 0: (one_out_ref, 9), 3: (two_out_ref, 0), 2: (two_out_ref, 9)}

    def partial(k, c, j):
        h = NODES // LANES + 3 * k + j
        at = 2 * c * ALL_ROWS + h // 2
        cols = pl.ds((h % 2) * LANES, LANES)
        return total[pl.ds(at, 1), cols] + total[pl.ds(at + ALL_ROWS, 1), cols]

    for m in range(4):
        for c in range(3):
            for j in range(3):
                low, high = partial(m, c, j), partial(m + 4, c, j)
                for label, x in ((m, jnp.where(second, high, low)), (m + 4, jnp.where(second, low, high))):
                    ref, base = target[label]
                    ref[pl.ds(base + c * 3 + j, 1), :] = x


def spread_kernel(own_ref, swap_ref, one_ref, two_ref, last_ref, send_ref, out_ref, lo, up):
    lowers, uppers = lower_parts(), upper_parts(OWN_ROWS)
    index = by_label(send_ref[...])
    lo[...] = (index & (WIDE - 1)).astype(F32)
    up[...] = (index >> 8).astype(F32)
    source = {0: (swap_ref, 27), 1: (one_ref, 0), 2: (one_ref, 18), 3: (two_ref, 0),
              4: (last_ref, 0), 5: (last_ref, 9), 6: (last_ref, 18), 7: (last_ref, 27)}
    hot, put = [], []
    for m in range(8):
        ref, base = source[m]
        for j in range(3):
            cols = pl.ds(j * LANES, LANES)
            hot.append(one_hot(lowers, lo[pl.ds(m, 1), cols]))
            values = [x for c in range(3) for x in split(ref[pl.ds(base + c * 3 + j, 1), :])]
            put.append(placed(uppers, up[pl.ds(m, 1), cols], values, OWN_ROWS))
    total = None
    for g in range(0, 24, 2):
        part = lax.dot_general(jnp.concatenate(put[g:g + 2], axis=1), jnp.concatenate(hot[g:g + 2], axis=1),
                               (((1,), (1,)), ((), ())), preferred_element_type=F32)
        total = part if total is None else total + part
    for c in range(3):
        for u in range(OWN_ROWS):
            q = 2 * c * OWN_ROWS + u
            out_ref[pl.ds(c, 1), pl.ds(u * WIDE, WIDE)] = (
                total[q:q + 1, :] + total[q + OWN_ROWS:q + OWN_ROWS + 1, :] + own_ref[pl.ds(c * OWN_ROWS + u, 1), :]
            )


def across(x):
    return lax.ppermute(x, "dom", [(i, i ^ 1) for i in range(lax.axis_size("dom"))])


def along(x, o):
    n = lax.axis_size("dom")
    route = {i: i + (2 * o if i % 2 == 0 else -2 * o) for i in range(n)}
    spare = sorted(set(range(n)) - set(route.values()))
    for i in range(n):
        if route[i] not in range(n):
            route[i] = min(spare, key=lambda j: (abs(j - i), j))
            spare.remove(route[i])
    return lax.ppermute(x, "dom", list(route.items()))


def in_hbm(x):
    return pltpu.with_memory_space_constraint(x, pltpu.HBM)


def params(kib):
    return pltpu.CompilerParams(vmem_limit_bytes=kib * 1024)


def body(field, blocks, connectivity, send_nodes, live_blocks):
    f = lambda *s: jax.ShapeDtypeStruct(s, F32)
    swap, out, field_near, conn_near = pl.pallas_call(
        pick_kernel,
        out_shape=(f(45, LANES), f(27, LANES), pltpu.VMEM((3, NODES), F32), pltpu.VMEM((10, ELEMS), jnp.int32)),
        in_specs=[HBM] * 3,
        out_specs=(VMEM,) * 4,
        scratch_shapes=[pltpu.VMEM((8, GHOST), jnp.int32), pltpu.SemaphoreType.DMA((3,))],
        compiler_params=params(1024),
        name="pick",
    )(in_hbm(field), in_hbm(send_nodes), in_hbm(connectivity))
    near = across(swap)
    one = along(jnp.concatenate([out[:9], near[9:18], out[9:18], near[18:27]]), 1)
    two = along(jnp.concatenate([out[18:], near[27:]]), 2)
    last = across(jnp.concatenate([one[18:], two[18:]]))
    smem = pl.BlockSpec(memory_space=pltpu.SMEM)
    prep = pl.pallas_call(
        prep_kernel,
        out_shape=(pltpu.VMEM((NBLK, 30, 30, BLK), BF16), pltpu.VMEM((NBLK, 30 * TILES, 8, LANES), F32),
                   pltpu.VMEM((NBLK, 10, BLK), F32), pltpu.VMEM((NBLK, 10, BLK), F32)),
        in_specs=[smem, VMEM, VMEM, VMEM, HBM],
        out_specs=(VMEM,) * 4,
        scratch_shapes=[pltpu.SemaphoreType.DMA((NBLK,)), pltpu.VMEM((table_rows(OWN_ROWS), WIDE), F32)],
        compiler_params=params(4096),
        cost_estimate=pl.CostEstimate(flops=2 * 10**10, bytes_accessed=2**23, transcendentals=0),
        name="prep",
    )
    stiff, sums, lo, up = prep(in_hbm(live_blocks), field_near, conn_near, near, in_hbm(blocks))
    own, swap, one_out, two_out = pl.pallas_call(
        main_kernel,
        out_shape=(f(3 * OWN_ROWS, WIDE), f(36, LANES), f(18, LANES), f(18, LANES)),
        in_specs=[smem] + [VMEM] * 8,
        out_specs=(VMEM,) * 4,
        scratch_shapes=[
            pltpu.VMEM((table_rows(GHOST_ROWS), WIDE), F32),
            pltpu.VMEM((30, BLK), F32),
            pltpu.VMEM((30, BLK), F32),
            pltpu.VMEM((30, BLK), F32),
            pltpu.VMEM((table_rows(ALL_ROWS), WIDE), F32),
        ],
        compiler_params=params(16384),
        cost_estimate=pl.CostEstimate(flops=2 * 10**10, bytes_accessed=2**23, transcendentals=0),
        name="main",
    )(in_hbm(live_blocks), near, one, two, last, stiff, sums, lo, up)
    swapped = across(swap)
    one_in = along(jnp.concatenate([one_out, swapped[:18]]), -1)
    two_in = along(jnp.concatenate([two_out, swapped[18:27]]), -2)
    back = across(jnp.concatenate([one_in[9:18], one_in[27:], two_in[9:]]))
    return pl.pallas_call(
        spread_kernel,
        out_shape=f(3, NODES),
        in_specs=[VMEM] * 6,
        out_specs=VMEM,
        scratch_shapes=[
            pltpu.VMEM((8, GHOST), F32),
            pltpu.VMEM((8, GHOST), F32),
        ],
        compiler_params=params(8192),
        name="spread",
    )(own, swapped, one_in, two_in, back, send_nodes)


def solution(mesh):
    return jax.shard_map(
        body,
        mesh=mesh,
        in_specs=(P(None, "dom"), P(None, None, "dom"), P(None, "dom"), P(None, "dom"), P()),
        out_specs=P(None, "dom"),
        check_vma=False,
    )
```

```python
import jax
import jax.numpy as jnp
from jax import lax
from jax.experimental import pallas as pl
from jax.experimental.pallas import tpu as pltpu
from jax.sharding import PartitionSpec as P


F32 = jnp.float32
BF16 = jnp.bfloat16
LANES = 128
WIDE = 256
BLK = 512
ELEMS = 4096
NBLK = ELEMS // BLK
NODES = 5632
GHOST = 384
SLOTS = NODES + 8 * GHOST
OWN_ROWS = NODES // WIDE
ALL_ROWS = SLOTS // WIDE
GHOST_ROWS = ALL_ROWS - OWN_ROWS
TILES = BLK // LANES
UNROLL = 2
VMEM = pl.BlockSpec(memory_space=pltpu.VMEM)
HBM = pl.BlockSpec(memory_space=pltpu.HBM)


def pad16(n):
    return -(-n // 16) * 16


def iota_rows(rows):
    return lax.broadcasted_iota(jnp.int32, (rows, LANES), 0)


def row_upper(rows, first, count):
    q = iota_rows(count) + first
    u = q
    for s in range(1, 6):
        u = jnp.where(q >= s * rows, q - s * rows, u)
    return jnp.where(q >= 6 * rows, -1, u).astype(F32)


def table_rows(rows):
    return pad16(6 * rows)


def select_parts(rows):
    per = 2 * rows
    out, seen = [], {}
    for g in range(-(-3 * per // 8)):
        for c in sorted({min(8 * g // per, 2), min((8 * g + 7) // per, 2)}):
            key = (max(8 * g, c * per) - c * per, min(8 * g + 8, c * per + per) - c * per, (c * per) % 8)
            if key not in seen:
                upper = row_upper(rows, 8 * g, 8)
                q = iota_rows(8) + 8 * g
                if 8 * g < c * per or 8 * g + 8 > c * per + per:
                    upper = jnp.where((q >= c * per) & (q < c * per + per), upper, -1.0)
                seen[key] = upper
            out.append((g, c, key))
    return out, seen


def select_sums(parts, row, got, lanes):
    order, uppers = parts
    here = jnp.broadcast_to(row, (8, LANES))
    hits, sums = {}, [jnp.zeros((8, LANES), F32)] * 3
    for g, c, key in order:
        if key not in hits:
            hits[key] = uppers[key] == here
        sums[c] = jnp.where(hits[key], got[8 * g:8 * g + 8, lanes:lanes + LANES], sums[c])
    return sums


def fill(tf, rows, x, c, h):
    hi, low = split(x)
    for part, y in ((0, hi), (1, low)):
        tf[pl.ds((c * 2 + part) * rows + h // 2, 1), pl.ds((h % 2) * LANES, LANES)] = y


def lower_parts():
    return [(iota_rows(16) + 16 * g).astype(F32).astype(BF16) for g in range(WIDE // 16)]


def upper_parts(rows):
    return [row_upper(rows, 16 * g, 16).astype(BF16) for g in range(pad16(6 * rows) // 16)]


def wide(row):
    return jnp.broadcast_to(row, (16, LANES)).astype(BF16)


def one_hot(parts, row):
    here, one, zero = wide(row), jnp.ones((16, LANES), BF16), jnp.zeros((16, LANES), BF16)
    return jnp.concatenate([jnp.where(part == here, one, zero) for part in parts], axis=0)


def split(x):
    hi = x.astype(BF16).astype(F32)
    return hi, x - hi


def placed(uppers, row, values, rows):
    here, zero = wide(row), jnp.zeros((16, LANES), BF16)
    values = [wide(v) for v in values]
    out = []
    for g, upper in enumerate(uppers):
        first, last = 16 * g // rows, (16 * g + 15) // rows
        value = values[min(first, 5)]
        if last != first and last <= 5:
            cut = (first + 1) * rows - 16 * g
            head = iota_rows(16).astype(F32).astype(BF16) < jnp.full((16, LANES), cut, BF16)
            value = jnp.where(head, value, values[last])
        out.append(jnp.where(upper == here, value, zero))
    return jnp.concatenate(out, axis=0)


def side():
    return lax.rem(lax.axis_index("dom"), 2)


def own_live(live_ref):
    here = lax.broadcasted_iota(jnp.int32, (1, LANES), 1) == lax.axis_index("dom")
    return jnp.sum(jnp.where(here, live_ref[...].astype(F32), 0.0)).astype(jnp.int32)


def by_label(x):
    return jnp.where(side() == 1, pltpu.roll(x, 4, axis=0), x)


def pick_kernel(field_hbm, send_hbm, conn_hbm, live_hbm, swap_ref, out_ref, field_ref, conn_ref, live_ref, send_ref, sem):
    copies = [pltpu.make_async_copy(field_hbm, field_ref, sem.at[0]), pltpu.make_async_copy(send_hbm, send_ref, sem.at[1]),
              pltpu.make_async_copy(conn_hbm, conn_ref, sem.at[2]), pltpu.make_async_copy(live_hbm, live_ref, sem.at[3])]
    for copy in copies:
        copy.start()
    copies[0].wait()
    copies[1].wait()
    place = {0: (swap_ref, 0), 4: (swap_ref, 9), 5: (swap_ref, 18), 6: (swap_ref, 27), 7: (swap_ref, 36),
             1: (out_ref, 0), 2: (out_ref, 9), 3: (out_ref, 18)}
    for j in range(3):
        index = by_label(send_ref[:, pl.ds(j * LANES, LANES)])
        upper, lower = index >> 7, index & 127
        total = [jnp.zeros((8, LANES), F32) for _ in range(3)]
        for h in range(NODES // LANES):
            hit = upper == h
            for c in range(3):
                row = jnp.broadcast_to(field_ref[pl.ds(c, 1), pl.ds(h * LANES, LANES)], (8, LANES))
                total[c] = jnp.where(hit, jnp.take_along_axis(row, lower, axis=1), total[c])
        for c in range(3):
            for m in range(8):
                ref, base = place[m]
                ref[pl.ds(base + c * 3 + j, 1), :] = total[c][m:m + 1, :]
    copies[2].wait()
    copies[3].wait()


def prep_kernel(live_ref, field_ref, conn_ref, after_ref, blocks_hbm, stiff_ref, sums_ref, lo_ref, up_ref, sem, tf):
    del after_ref
    n = own_live(live_ref)

    def fetch(b):
        return pltpu.make_async_copy(blocks_hbm.at[:, :, pl.ds(pl.multiple_of(b * BLK, BLK), BLK)], stiff_ref.at[b], sem.at[b])

    def start(b, _):
        fetch(b).start()
        return 0

    def wait(b, _):
        fetch(b).wait()
        return 0

    lax.fori_loop(0, n, start, 0)
    used = 6 * OWN_ROWS
    tf[pl.ds(used // 8 * 8, tf.shape[0] - used // 8 * 8), :] = jnp.zeros((tf.shape[0] - used // 8 * 8, WIDE), F32)
    for h in range(NODES // LANES):
        x = field_ref[:, pl.ds(h * LANES, LANES)]
        for c in range(3):
            fill(tf, OWN_ROWS, x[c:c + 1, :], c, h)
    table = tf[...].astype(BF16)
    lowers, parts = lower_parts(), select_parts(OWN_ROWS)

    def step(b, _):
        block = pl.ds(pl.multiple_of(b * BLK, BLK), BLK)
        index = conn_ref[:, block]
        lo_ref[b] = (index & (WIDE - 1)).astype(F32)
        up_ref[b] = (index >> 8).astype(F32)
        for a in range(10):
            for t2 in range(TILES // 2):
                cols = [pl.ds((2 * t2 + s) * LANES, LANES) for s in range(2)]
                hot = jnp.concatenate([one_hot(lowers, lo_ref[b, pl.ds(a, 1), c]) for c in cols], axis=1)
                got = jnp.dot(table, hot, preferred_element_type=F32)
                for s in range(2):
                    sums = select_sums(parts, up_ref[b, pl.ds(a, 1), cols[s]], got, s * LANES)
                    for c in range(3):
                        sums_ref[b, (a * TILES + 2 * t2 + s) * 3 + c] = sums[c]
        return 0

    lax.fori_loop(0, n, step, 0)
    lax.fori_loop(0, n, wait, 0)


def main_kernel(live_ref, near_ref, one_ref, two_ref, last_ref, stiff_ref, sums_ref, lo_ref, up_ref,
                own_ref, swap_ref, one_out_ref, two_out_ref, tf, vals, high, low, total):
    n = own_live(live_ref)
    second = side() == 1

    used = 6 * GHOST_ROWS
    tf[pl.ds(used, tf.shape[0] - used), :] = jnp.zeros((tf.shape[0] - used, WIDE), F32)
    source = {0: (one_ref, 9), 1: (one_ref, 0), 2: (two_ref, 9), 3: (two_ref, 0),
              4: (near_ref, 0), 5: (last_ref, 9), 6: (last_ref, 0), 7: (last_ref, 18)}
    ghost = [source[m][0][pl.ds(source[m][1], 9), :] for m in range(8)]
    for k in range(8):
        bundle = jnp.where(second, ghost[k ^ 4], ghost[k])
        for c in range(3):
            for j in range(3):
                q = c * 3 + j
                fill(tf, GHOST_ROWS, bundle[q:q + 1, :], c, 3 * k + j)
    table = tf[...].astype(BF16)
    total[...] = jnp.zeros_like(total)
    lowers, uppers, parts = lower_parts(), upper_parts(ALL_ROWS), select_parts(GHOST_ROWS)

    def gather(b, half, hots, vals):
        def chunk(a):
            cols = [pl.ds((2 * half + s) * LANES, LANES) for s in range(2)]
            hots[a] = hot = jnp.concatenate([one_hot(lowers, lo_ref[b, pl.ds(a, 1), c]) for c in cols], axis=1).astype(jnp.float8_e4m3fn)
            got = jnp.dot(table, hot, preferred_element_type=F32)
            for s in range(2):
                sums = select_sums(parts, up_ref[b, pl.ds(a, 1), cols[s]] - OWN_ROWS, got, s * LANES)
                for c in range(3):
                    both = sums[c] + sums_ref[b, (a * TILES + 2 * half + s) * 3 + c]
                    vals[pl.ds(c * 10 + a, 1), pl.ds(s * LANES, LANES)] = jnp.sum(both, axis=0, keepdims=True)

        return [lambda a=a: chunk(a) for a in range(10)]

    def apply(b, half, vals, high, low):
        def row(i):
            for s in range(2):
                cols = pl.ds(s * LANES, LANES)
                k = stiff_ref[b, i, :, pl.ds((2 * half + s) * LANES, LANES)].astype(F32)
                high[pl.ds(i, 1), cols] = jnp.sum(k * vals[:, cols], axis=0, keepdims=True)

        def finish():
            force = jnp.where(b < n, high[...], 0.0)
            high[...], low[...] = split(force)

        return [lambda i=i: row(i) for i in range(30)] + [finish]

    def scatter(b, half, hots, high, low, acc):
        def chunk(a):
            put = []
            for s in range(2):
                cols = pl.ds(s * LANES, LANES)
                values = [ref[pl.ds(c * 10 + a, 1), cols] for c in range(3) for ref in (high, low)]
                row = up_ref[b, pl.ds(a, 1), pl.ds((2 * half + s) * LANES, LANES)]
                put.append(placed(uppers, row, values, ALL_ROWS))
            hot = hots[a]
            part = lax.dot_general(jnp.concatenate(put, axis=1), hot, (((1,), (1,)), ((), ())), preferred_element_type=F32)
            acc[0] = part if acc[0] is None else acc[0] + part

        return [lambda a=a: chunk(a) for a in range(10)]

    def together(*streams):
        pieces = [((i + 1) / len(stream), k, i) for k, stream in enumerate(streams) for i in range(len(stream))]
        for _, k, i in sorted(pieces):
            streams[k][i]()

    def step(trip, _):
        units = [(UNROLL * trip + k, half) for k in range(UNROLL) for half in range(2)]
        hots = [[None] * 10 for _ in units]
        acc = [None]
        buffers = [(vals.at[k], high.at[k], low.at[k]) for k in range(len(units))]
        order = [("gather", k) for k in range(len(units))] + [("apply", 0)]
        for k in range(len(units)):
            order += ([("apply", k + 1)] if k + 1 < len(units) else []) + [("scatter", k)]
        for kind, k in order:
            streams = []
            v, h, w = buffers[k]
            if kind == "scatter":
                streams.append(scatter(*units[k], hots[k], h, w, acc))
            elif kind == "apply":
                streams.append(apply(*units[k], v, h, w))
            else:
                streams.append(gather(*units[k], hots[k], v))
            together(*streams)
        total[...] += acc[0]
        return 0

    lax.fori_loop(0, lax.div(n + (UNROLL - 1), UNROLL), step, 0)

    for c in range(3):
        base = 2 * c * ALL_ROWS
        own_ref[pl.ds(c * OWN_ROWS, OWN_ROWS), :] = total[pl.ds(base, OWN_ROWS), :] + total[pl.ds(base + ALL_ROWS, OWN_ROWS), :]
    target = {6: (swap_ref, 0), 5: (swap_ref, 9), 7: (swap_ref, 18), 4: (swap_ref, 27),
              1: (one_out_ref, 0), 0: (one_out_ref, 9), 3: (two_out_ref, 0), 2: (two_out_ref, 9)}

    def partial(k, c, j):
        h = NODES // LANES + 3 * k + j
        at = 2 * c * ALL_ROWS + h // 2
        cols = pl.ds((h % 2) * LANES, LANES)
        return total[pl.ds(at, 1), cols] + total[pl.ds(at + ALL_ROWS, 1), cols]

    for m in range(4):
        for c in range(3):
            for j in range(3):
                low, high = partial(m, c, j), partial(m + 4, c, j)
                for label, x in ((m, jnp.where(second, high, low)), (m + 4, jnp.where(second, low, high))):
                    ref, base = target[label]
                    ref[pl.ds(base + c * 3 + j, 1), :] = x


def spread_kernel(own_ref, swap_ref, one_ref, two_ref, last_ref, send_ref, out_ref, lo, up):
    lowers, uppers = lower_parts(), upper_parts(OWN_ROWS)
    index = by_label(send_ref[...])
    lo[...] = (index & (WIDE - 1)).astype(F32)
    up[...] = (index >> 8).astype(F32)
    source = {0: (swap_ref, 27), 1: (one_ref, 0), 2: (one_ref, 18), 3: (two_ref, 0),
              4: (last_ref, 0), 5: (last_ref, 9), 6: (last_ref, 18), 7: (last_ref, 27)}
    hot, put = [], []
    for m in range(8):
        ref, base = source[m]
        for j in range(3):
            cols = pl.ds(j * LANES, LANES)
            hot.append(one_hot(lowers, lo[pl.ds(m, 1), cols]))
            values = [x for c in range(3) for x in split(ref[pl.ds(base + c * 3 + j, 1), :])]
            put.append(placed(uppers, up[pl.ds(m, 1), cols], values, OWN_ROWS))
    total = None
    for g in range(0, 24, 2):
        part = lax.dot_general(jnp.concatenate(put[g:g + 2], axis=1), jnp.concatenate(hot[g:g + 2], axis=1),
                               (((1,), (1,)), ((), ())), preferred_element_type=F32)
        total = part if total is None else total + part
    for c in range(3):
        for u in range(OWN_ROWS):
            q = 2 * c * OWN_ROWS + u
            out_ref[pl.ds(c, 1), pl.ds(u * WIDE, WIDE)] = (
                total[q:q + 1, :] + total[q + OWN_ROWS:q + OWN_ROWS + 1, :] + own_ref[pl.ds(c * OWN_ROWS + u, 1), :]
            )


def across(x):
    return lax.ppermute(x, "dom", [(i, i ^ 1) for i in range(lax.axis_size("dom"))])


def along(x, o):
    n = lax.axis_size("dom")
    route = {i: i + (2 * o if i % 2 == 0 else -2 * o) for i in range(n)}
    spare = sorted(set(range(n)) - set(route.values()))
    for i in range(n):
        if route[i] not in range(n):
            route[i] = min(spare, key=lambda j: (abs(j - i), j))
            spare.remove(route[i])
    return lax.ppermute(x, "dom", list(route.items()))


def in_hbm(x):
    return pltpu.with_memory_space_constraint(x, pltpu.HBM)


def params(kib):
    return pltpu.CompilerParams(vmem_limit_bytes=kib * 1024)


def rows_f32(*shape):
    return jax.ShapeDtypeStruct(shape, F32)


def prep_call():
    return pl.pallas_call(
        prep_kernel,
        out_shape=(pltpu.VMEM((NBLK, 30, 30, BLK), BF16), pltpu.VMEM((NBLK, 30 * TILES, 8, LANES), F32),
                   pltpu.VMEM((NBLK, 10, BLK), F32), pltpu.VMEM((NBLK, 10, BLK), F32)),
        in_specs=[VMEM] * 4 + [HBM],
        out_specs=(VMEM,) * 4,
        scratch_shapes=[pltpu.SemaphoreType.DMA((NBLK,)), pltpu.VMEM((table_rows(OWN_ROWS), WIDE), F32)],
        compiler_params=params(4096),
        cost_estimate=pl.CostEstimate(flops=2 * 10**10, bytes_accessed=2**23, transcendentals=0),
        name="prep",
    )


def main_call():
    return pl.pallas_call(
        main_kernel,
        out_shape=(rows_f32(3 * OWN_ROWS, WIDE), rows_f32(36, LANES), rows_f32(18, LANES), rows_f32(18, LANES)),
        in_specs=[VMEM] * 9,
        out_specs=(VMEM,) * 4,
        scratch_shapes=[
            pltpu.VMEM((table_rows(GHOST_ROWS), WIDE), F32),
            pltpu.VMEM((2 * UNROLL, 30, BLK // 2), F32),
            pltpu.VMEM((2 * UNROLL, 30, BLK // 2), F32),
            pltpu.VMEM((2 * UNROLL, 30, BLK // 2), F32),
            pltpu.VMEM((table_rows(ALL_ROWS), WIDE), F32),
        ],
        compiler_params=params(16384),
        cost_estimate=pl.CostEstimate(flops=2 * 10**10, bytes_accessed=2**23, transcendentals=0),
        name="main",
    )


def body(field, blocks, connectivity, send_nodes, live_blocks):
    swap, out, field_near, conn_near, live = pl.pallas_call(
        pick_kernel,
        out_shape=(rows_f32(45, LANES), rows_f32(27, LANES), pltpu.VMEM((3, NODES), F32), pltpu.VMEM((10, ELEMS), jnp.int32),
                   pltpu.VMEM((1, LANES), jnp.int32)),
        in_specs=[HBM] * 4,
        out_specs=(VMEM,) * 5,
        scratch_shapes=[pltpu.VMEM((8, GHOST), jnp.int32), pltpu.SemaphoreType.DMA((4,))],
        compiler_params=params(1024),
        name="pick",
    )(in_hbm(field), in_hbm(send_nodes), in_hbm(connectivity), in_hbm(live_blocks.reshape(1, LANES)))
    near = across(swap)
    one = along(jnp.concatenate([out[:9], near[9:18], out[9:18], near[18:27]]), 1)
    two = along(jnp.concatenate([out[18:], near[27:]]), 2)
    last = across(jnp.concatenate([one[18:], two[18:]]))
    stiff, sums, lo, up = prep_call()(live, field_near, conn_near, near, in_hbm(blocks))
    own, swap, one_out, two_out = main_call()(live, near, one, two, last, stiff, sums, lo, up)
    swapped = across(swap)
    one_in = along(jnp.concatenate([one_out, swapped[:18]]), -1)
    two_in = along(jnp.concatenate([two_out, swapped[18:27]]), -2)
    back = across(jnp.concatenate([one_in[9:18], one_in[27:], two_in[9:]]))
    return pl.pallas_call(
        spread_kernel,
        out_shape=rows_f32(3, NODES),
        in_specs=[VMEM] * 6,
        out_specs=VMEM,
        scratch_shapes=[
            pltpu.VMEM((8, GHOST), F32),
            pltpu.VMEM((8, GHOST), F32),
        ],
        compiler_params=params(8192),
        name="spread",
    )(own, swapped, one_in, two_in, back, send_nodes)


def solution(mesh):
    return jax.shard_map(
        body,
        mesh=mesh,
        in_specs=(P(None, "dom"), P(None, None, "dom"), P(None, "dom"), P(None, "dom"), P()),
        out_specs=P(None, "dom"),
        check_vma=False,
    )
```

```python
import jax
import jax.numpy as jnp
from jax import lax
from jax.experimental import pallas as pl
from jax.experimental.pallas import tpu as pltpu
from jax.sharding import PartitionSpec as P


F32 = jnp.float32
BF16 = jnp.bfloat16
F8 = jnp.float8_e4m3fn
LANES = 128
WIDE = 256
BLK = 512
ELEMS = 4096
NBLK = ELEMS // BLK
NODES = 5632
GHOST = 384
SLOTS = NODES + 8 * GHOST
OWN_ROWS = NODES // WIDE
ALL_ROWS = SLOTS // WIDE
GHOST_ROWS = ALL_ROWS - OWN_ROWS
GHOST_PAD = 16
OWN_PAD = 24
TILES = BLK // LANES
UNROLL = 2
VMEM = pl.BlockSpec(memory_space=pltpu.VMEM)
HBM = pl.BlockSpec(memory_space=pltpu.HBM)


def pad16(n):
    return -(-n // 16) * 16


def iota_rows(rows):
    return lax.broadcasted_iota(jnp.int32, (rows, LANES), 0)


def row_upper(rows, first, count):
    q = iota_rows(count) + first
    u = q
    for s in range(1, 6):
        u = jnp.where(q >= s * rows, q - s * rows, u)
    return jnp.where(q >= 6 * rows, -1, u).astype(F32)


def table_rows(rows):
    return pad16(6 * rows)


def select_parts(rows):
    per = 2 * rows
    out, seen = [], {}
    for g in range(-(-3 * per // 8)):
        for c in sorted({min(8 * g // per, 2), min((8 * g + 7) // per, 2)}):
            key = (max(8 * g, c * per) - c * per, min(8 * g + 8, c * per + per) - c * per, (c * per) % 8)
            if key not in seen:
                upper = row_upper(rows, 8 * g, 8)
                q = iota_rows(8) + 8 * g
                if 8 * g < c * per or 8 * g + 8 > c * per + per:
                    upper = jnp.where((q >= c * per) & (q < c * per + per), upper, -1.0)
                seen[key] = upper
            out.append((g, c, key))
    return out, seen


def select_sums(parts, row, got, lanes):
    order, uppers = parts
    here = jnp.broadcast_to(row, (8, LANES))
    hits, sums = {}, [jnp.zeros((8, LANES), F32)] * 3
    for g, c, key in order:
        if key not in hits:
            hits[key] = uppers[key] == here
        sums[c] = jnp.where(hits[key], got[8 * g:8 * g + 8, lanes:lanes + LANES], sums[c])
    return sums


def fill(tf, rows, x, c, h):
    hi, low = split(x)
    for part, y in ((0, hi), (1, low)):
        tf[pl.ds((c * 2 + part) * rows + h // 2, 1), pl.ds((h % 2) * LANES, LANES)] = y


def lower_parts():
    return [(iota_rows(16) + 16 * g).astype(F32).astype(BF16) for g in range(WIDE // 16)]


def upper_parts(rows):
    return [row_upper(rows, 16 * g, 16).astype(BF16) for g in range(pad16(6 * rows) // 16)]


def wide(row):
    return jnp.broadcast_to(row, (16, LANES)).astype(BF16)


def one_hot(parts, row):
    here, one, zero = wide(row), jnp.ones((16, LANES), BF16), jnp.zeros((16, LANES), BF16)
    return jnp.concatenate([jnp.where(part == here, one, zero) for part in parts], axis=0)


def split(x):
    hi = x.astype(BF16).astype(F32)
    return hi, x - hi


def placed(uppers, row, values, rows):
    here, zero = wide(row), jnp.zeros((16, LANES), BF16)
    values = [wide(v) for v in values]
    out = []
    for g, upper in enumerate(uppers):
        first, last = 16 * g // rows, (16 * g + 15) // rows
        value = values[min(first, 5)]
        if last != first and last <= 5:
            cut = (first + 1) * rows - 16 * g
            head = iota_rows(16).astype(F32).astype(BF16) < jnp.full((16, LANES), cut, BF16)
            value = jnp.where(head, value, values[last])
        out.append(jnp.where(upper == here, value, zero))
    return jnp.concatenate(out, axis=0)


def side():
    return lax.rem(lax.axis_index("dom"), 2)


def own_live(live_ref):
    here = lax.broadcasted_iota(jnp.int32, (1, LANES), 1) == lax.axis_index("dom")
    return jnp.sum(jnp.where(here, live_ref[...].astype(F32), 0.0)).astype(jnp.int32)


def by_label(x):
    return jnp.where(side() == 1, pltpu.roll(x, 4, axis=0), x)


def pick_kernel(field_hbm, send_hbm, conn_hbm, live_hbm, swap_ref, out_ref, field_ref, conn_ref, live_ref, send_ref, sem):
    copies = [pltpu.make_async_copy(field_hbm, field_ref, sem.at[0]), pltpu.make_async_copy(send_hbm, send_ref, sem.at[1]),
              pltpu.make_async_copy(conn_hbm, conn_ref, sem.at[2]), pltpu.make_async_copy(live_hbm, live_ref, sem.at[3])]
    for copy in copies:
        copy.start()
    copies[0].wait()
    copies[1].wait()
    place = {0: (swap_ref, 0), 4: (swap_ref, 9), 5: (swap_ref, 18), 6: (swap_ref, 27), 7: (swap_ref, 36),
             1: (out_ref, 0), 2: (out_ref, 9), 3: (out_ref, 18)}
    for j in range(3):
        index = by_label(send_ref[:, pl.ds(j * LANES, LANES)])
        upper, lower = index >> 7, index & 127
        total = [jnp.zeros((8, LANES), F32) for _ in range(3)]
        for h in range(NODES // LANES):
            hit = upper == h
            for c in range(3):
                row = jnp.broadcast_to(field_ref[pl.ds(c, 1), pl.ds(h * LANES, LANES)], (8, LANES))
                total[c] = jnp.where(hit, jnp.take_along_axis(row, lower, axis=1), total[c])
        for c in range(3):
            for m in range(8):
                ref, base = place[m]
                ref[pl.ds(base + c * 3 + j, 1), :] = total[c][m:m + 1, :]
    copies[2].wait()
    copies[3].wait()


def prep_kernel(live_ref, field_ref, conn_ref, after_ref, blocks_hbm, stiff_ref, sums_ref, lo_ref, up_ref, sem, tf):
    del after_ref
    n = own_live(live_ref)

    def fetch(b):
        return pltpu.make_async_copy(blocks_hbm.at[:, :, pl.ds(pl.multiple_of(b * BLK, BLK), BLK)], stiff_ref.at[b], sem.at[b])

    def start(b, _):
        fetch(b).start()
        return 0

    def wait(b, _):
        fetch(b).wait()
        return 0

    lax.fori_loop(0, n, start, 0)
    used = 6 * OWN_ROWS
    tf[pl.ds(used // 8 * 8, tf.shape[0] - used // 8 * 8), :] = jnp.zeros((tf.shape[0] - used // 8 * 8, WIDE), F32)
    for h in range(NODES // LANES):
        x = field_ref[:, pl.ds(h * LANES, LANES)]
        for c in range(3):
            fill(tf, OWN_ROWS, x[c:c + 1, :], c, h)
    table = tf[...].astype(BF16)
    lowers, parts = lower_parts(), select_parts(OWN_ROWS)

    def step(b, _):
        block = pl.ds(pl.multiple_of(b * BLK, BLK), BLK)
        index = conn_ref[:, block]
        lo_ref[b] = (index & (WIDE - 1)).astype(F32)
        up_ref[b] = (index >> 8).astype(F32)
        for a in range(10):
            for t2 in range(TILES // 2):
                cols = [pl.ds((2 * t2 + s) * LANES, LANES) for s in range(2)]
                hot = jnp.concatenate([one_hot(lowers, lo_ref[b, pl.ds(a, 1), c]) for c in cols], axis=1)
                got = jnp.dot(table, hot, preferred_element_type=F32)
                for s in range(2):
                    sums = select_sums(parts, up_ref[b, pl.ds(a, 1), cols[s]], got, s * LANES)
                    for c in range(3):
                        sums_ref[b, (a * TILES + 2 * t2 + s) * 3 + c] = sums[c]
        return 0

    lax.fori_loop(0, n, step, 0)
    lax.fori_loop(0, n, wait, 0)


def main_kernel(live_ref, near_ref, one_ref, two_ref, last_ref, stiff_ref, sums_ref, lo_ref, up_ref,
                swap_ref, one_out_ref, two_out_ref, high_ref, low_ref, tf, vals, high, low, total):
    n = own_live(live_ref)
    second = side() == 1

    used = 6 * GHOST_ROWS
    tf[pl.ds(used, tf.shape[0] - used), :] = jnp.zeros((tf.shape[0] - used, WIDE), F32)
    source = {0: (one_ref, 9), 1: (one_ref, 0), 2: (two_ref, 9), 3: (two_ref, 0),
              4: (near_ref, 0), 5: (last_ref, 9), 6: (last_ref, 0), 7: (last_ref, 18)}
    ghost = [source[m][0][pl.ds(source[m][1], 9), :] for m in range(8)]
    for k in range(8):
        bundle = jnp.where(second, ghost[k ^ 4], ghost[k])
        for c in range(3):
            for j in range(3):
                q = c * 3 + j
                fill(tf, GHOST_ROWS, bundle[q:q + 1, :], c, 3 * k + j)
    table = tf[...].astype(BF16)
    total[...] = jnp.zeros_like(total)
    lowers, uppers, parts = lower_parts(), [iota_rows(16).astype(F32).astype(BF16)] * 6, select_parts(GHOST_ROWS)

    def gather(b, half, hots, vals):
        def chunk(a):
            cols = [pl.ds((2 * half + s) * LANES, LANES) for s in range(2)]
            hots[a] = hot = jnp.concatenate([one_hot(lowers, lo_ref[b, pl.ds(a, 1), c]) for c in cols], axis=1).astype(F8)
            got = jnp.dot(table, hot, preferred_element_type=F32)
            for s in range(2):
                sums = select_sums(parts, up_ref[b, pl.ds(a, 1), cols[s]] - OWN_ROWS, got, s * LANES)
                for c in range(3):
                    both = sums[c] + sums_ref[b, (a * TILES + 2 * half + s) * 3 + c]
                    vals[pl.ds(c * 10 + a, 1), pl.ds(s * LANES, LANES)] = jnp.sum(both, axis=0, keepdims=True)

        return [lambda a=a: chunk(a) for a in range(10)]

    def apply(b, half, vals, high, low):
        def row(i):
            for s in range(2):
                cols = pl.ds(s * LANES, LANES)
                k = stiff_ref[b, i, :, pl.ds((2 * half + s) * LANES, LANES)].astype(F32)
                high[pl.ds(i, 1), cols] = jnp.sum(k * vals[:, cols], axis=0, keepdims=True)

        def finish():
            force = jnp.where(b < n, high[...], 0.0)
            high[...], low[...] = split(force)
            high_ref[b, half], low_ref[b, half] = high[...], low[...]

        return [lambda i=i: row(i) for i in range(30)] + [finish]

    def scatter(b, half, hots, high, low, acc):
        def chunk(a):
            put = []
            for s in range(2):
                cols = pl.ds(s * LANES, LANES)
                values = [ref[pl.ds(c * 10 + a, 1), cols] for c in range(3) for ref in (high, low)]
                row = up_ref[b, pl.ds(a, 1), pl.ds((2 * half + s) * LANES, LANES)] - OWN_ROWS
                put.append(placed(uppers, row, values, GHOST_PAD))
            hot = hots[a]
            part = lax.dot_general(jnp.concatenate(put, axis=1), hot, (((1,), (1,)), ((), ())), preferred_element_type=F32)
            acc[0] = part if acc[0] is None else acc[0] + part

        return [lambda a=a: chunk(a) for a in range(10)]

    def together(*streams):
        pieces = [((i + 1) / len(stream), k, i) for k, stream in enumerate(streams) for i in range(len(stream))]
        for _, k, i in sorted(pieces):
            streams[k][i]()

    def step(trip, _):
        units = [(UNROLL * trip + k, half) for k in range(UNROLL) for half in range(2)]
        hots = [[None] * 10 for _ in units]
        acc = [None]
        buffers = [(vals.at[k], high.at[k], low.at[k]) for k in range(len(units))]
        order = [("gather", k) for k in range(len(units))] + [("apply", 0)]
        for k in range(len(units)):
            order += ([("apply", k + 1)] if k + 1 < len(units) else []) + [("scatter", k)]
        for kind, k in order:
            streams = []
            v, h, w = buffers[k]
            if kind == "scatter":
                streams.append(scatter(*units[k], hots[k], h, w, acc))
            elif kind == "apply":
                streams.append(apply(*units[k], v, h, w))
            else:
                streams.append(gather(*units[k], hots[k], v))
            together(*streams)
        total[...] += acc[0]
        return 0

    lax.fori_loop(0, lax.div(n + (UNROLL - 1), UNROLL), step, 0)

    target = {6: (swap_ref, 0), 5: (swap_ref, 9), 7: (swap_ref, 18), 4: (swap_ref, 27),
              1: (one_out_ref, 0), 0: (one_out_ref, 9), 3: (two_out_ref, 0), 2: (two_out_ref, 9)}

    def partial(k, c, j):
        h = 3 * k + j
        at = 2 * c * GHOST_PAD + h // 2
        cols = pl.ds((h % 2) * LANES, LANES)
        return total[pl.ds(at, 1), cols] + total[pl.ds(at + GHOST_PAD, 1), cols]

    for m in range(4):
        for c in range(3):
            for j in range(3):
                low, high = partial(m, c, j), partial(m + 4, c, j)
                for label, x in ((m, jnp.where(second, high, low)), (m + 4, jnp.where(second, low, high))):
                    ref, base = target[label]
                    ref[pl.ds(base + c * 3 + j, 1), :] = x


def finish_kernel(live_ref, lo_ref, up_ref, high_ref, low_ref, after_ref, own_ref, total):
    del after_ref
    n = own_live(live_ref)
    lowers, uppers = lower_parts(), upper_parts(OWN_PAD)[:3] * 3
    total[...] = jnp.zeros_like(total)

    def step(trip, _):
        acc = None
        for k in range(UNROLL):
            b = UNROLL * trip + k
            for half in range(2):
                for a in range(10):
                    put, hot = [], []
                    for s in range(2):
                        inner, outer = pl.ds(s * LANES, LANES), pl.ds((2 * half + s) * LANES, LANES)
                        hot.append(one_hot(lowers, lo_ref[b, pl.ds(a, 1), outer]))
                        values = [ref[b, half, pl.ds(c * 10 + a, 1), inner] for c in range(3) for ref in (high_ref, low_ref)]
                        put.append(placed(uppers, up_ref[b, pl.ds(a, 1), outer], values, OWN_PAD))
                    part = lax.dot_general(jnp.concatenate(put, axis=1), jnp.concatenate(hot, axis=1).astype(F8),
                                           (((1,), (1,)), ((), ())), preferred_element_type=F32)
                    acc = part if acc is None else acc + part
        total[...] += acc
        return 0

    lax.fori_loop(0, lax.div(n + (UNROLL - 1), UNROLL), step, 0)
    for c in range(3):
        base = 2 * c * OWN_PAD
        own_ref[pl.ds(c * OWN_ROWS, OWN_ROWS), :] = total[pl.ds(base, OWN_ROWS), :] + total[pl.ds(base + OWN_PAD, OWN_ROWS), :]


def spread_kernel(own_ref, swap_ref, one_ref, two_ref, last_ref, send_ref, out_ref, lo, up):
    lowers, uppers = lower_parts(), upper_parts(OWN_ROWS)
    index = by_label(send_ref[...])
    lo[...] = (index & (WIDE - 1)).astype(F32)
    up[...] = (index >> 8).astype(F32)
    source = {0: (swap_ref, 27), 1: (one_ref, 0), 2: (one_ref, 18), 3: (two_ref, 0),
              4: (last_ref, 0), 5: (last_ref, 9), 6: (last_ref, 18), 7: (last_ref, 27)}
    hot, put = [], []
    for m in range(8):
        ref, base = source[m]
        for j in range(3):
            cols = pl.ds(j * LANES, LANES)
            hot.append(one_hot(lowers, lo[pl.ds(m, 1), cols]))
            values = [x for c in range(3) for x in split(ref[pl.ds(base + c * 3 + j, 1), :])]
            put.append(placed(uppers, up[pl.ds(m, 1), cols], values, OWN_ROWS))
    total = None
    for g in range(0, 24, 2):
        part = lax.dot_general(jnp.concatenate(put[g:g + 2], axis=1), jnp.concatenate(hot[g:g + 2], axis=1),
                               (((1,), (1,)), ((), ())), preferred_element_type=F32)
        total = part if total is None else total + part
    for c in range(3):
        for u in range(OWN_ROWS):
            q = 2 * c * OWN_ROWS + u
            out_ref[pl.ds(c, 1), pl.ds(u * WIDE, WIDE)] = (
                total[q:q + 1, :] + total[q + OWN_ROWS:q + OWN_ROWS + 1, :] + own_ref[pl.ds(c * OWN_ROWS + u, 1), :]
            )


def across(x):
    return lax.ppermute(x, "dom", [(i, i ^ 1) for i in range(lax.axis_size("dom"))])


def along(x, o):
    n = lax.axis_size("dom")
    route = {i: i + (2 * o if i % 2 == 0 else -2 * o) for i in range(n)}
    spare = sorted(set(range(n)) - set(route.values()))
    for i in range(n):
        if route[i] not in range(n):
            route[i] = min(spare, key=lambda j: (abs(j - i), j))
            spare.remove(route[i])
    return lax.ppermute(x, "dom", list(route.items()))


def in_hbm(x):
    return pltpu.with_memory_space_constraint(x, pltpu.HBM)


def params(kib):
    return pltpu.CompilerParams(vmem_limit_bytes=kib * 1024)


def rows_f32(*shape):
    return jax.ShapeDtypeStruct(shape, F32)


def prep_call():
    return pl.pallas_call(
        prep_kernel,
        out_shape=(pltpu.VMEM((NBLK, 30, 30, BLK), BF16), pltpu.VMEM((NBLK, 30 * TILES, 8, LANES), F32),
                   pltpu.VMEM((NBLK, 10, BLK), F32), pltpu.VMEM((NBLK, 10, BLK), F32)),
        in_specs=[VMEM] * 4 + [HBM],
        out_specs=(VMEM,) * 4,
        scratch_shapes=[pltpu.SemaphoreType.DMA((NBLK,)), pltpu.VMEM((table_rows(OWN_ROWS), WIDE), F32)],
        compiler_params=params(4096),
        cost_estimate=pl.CostEstimate(flops=2 * 10**10, bytes_accessed=2**23, transcendentals=0),
        name="prep",
    )


def main_call():
    return pl.pallas_call(
        main_kernel,
        out_shape=(rows_f32(36, LANES), rows_f32(18, LANES), rows_f32(18, LANES),
                   pltpu.VMEM((NBLK, 2, 30, BLK // 2), F32), pltpu.VMEM((NBLK, 2, 30, BLK // 2), F32)),
        in_specs=[VMEM] * 9,
        out_specs=(VMEM,) * 5,
        scratch_shapes=[
            pltpu.VMEM((table_rows(GHOST_ROWS), WIDE), F32),
            pltpu.VMEM((2 * UNROLL, 30, BLK // 2), F32),
            pltpu.VMEM((2 * UNROLL, 30, BLK // 2), F32),
            pltpu.VMEM((2 * UNROLL, 30, BLK // 2), F32),
            pltpu.VMEM((6 * GHOST_PAD, WIDE), F32),
        ],
        compiler_params=params(16384),
        cost_estimate=pl.CostEstimate(flops=2 * 10**10, bytes_accessed=2**23, transcendentals=0),
        name="main",
    )


def finish_call():
    return pl.pallas_call(
        finish_kernel,
        out_shape=rows_f32(3 * OWN_ROWS, WIDE),
        in_specs=[VMEM] * 6,
        out_specs=VMEM,
        scratch_shapes=[pltpu.VMEM((6 * OWN_PAD, WIDE), F32)],
        compiler_params=params(12288),
        cost_estimate=pl.CostEstimate(flops=2 * 10**10, bytes_accessed=2**23, transcendentals=0),
        name="finish",
    )


def body(field, blocks, connectivity, send_nodes, live_blocks):
    swap, out, field_near, conn_near, live = pl.pallas_call(
        pick_kernel,
        out_shape=(rows_f32(45, LANES), rows_f32(27, LANES), pltpu.VMEM((3, NODES), F32), pltpu.VMEM((10, ELEMS), jnp.int32),
                   pltpu.VMEM((1, LANES), jnp.int32)),
        in_specs=[HBM] * 4,
        out_specs=(VMEM,) * 5,
        scratch_shapes=[pltpu.VMEM((8, GHOST), jnp.int32), pltpu.SemaphoreType.DMA((4,))],
        compiler_params=params(1024),
        name="pick",
    )(in_hbm(field), in_hbm(send_nodes), in_hbm(connectivity), in_hbm(live_blocks.reshape(1, LANES)))
    near = across(swap)
    one = along(jnp.concatenate([out[:9], near[9:18], out[9:18], near[18:27]]), 1)
    two = along(jnp.concatenate([out[18:], near[27:]]), 2)
    last = across(jnp.concatenate([one[18:], two[18:]]))
    stiff, sums, lo, up = prep_call()(live, field_near, conn_near, near, in_hbm(blocks))
    swap, one_out, two_out, high, low = main_call()(live, near, one, two, last, stiff, sums, lo, up)
    swapped = across(swap)
    one_in = along(jnp.concatenate([one_out, swapped[:18]]), -1)
    two_in = along(jnp.concatenate([two_out, swapped[18:27]]), -2)
    own = finish_call()(live, lo, up, high, low, swapped)
    back = across(jnp.concatenate([one_in[9:18], one_in[27:], two_in[9:]]))
    return pl.pallas_call(
        spread_kernel,
        out_shape=rows_f32(3, NODES),
        in_specs=[VMEM] * 6,
        out_specs=VMEM,
        scratch_shapes=[
            pltpu.VMEM((8, GHOST), F32),
            pltpu.VMEM((8, GHOST), F32),
        ],
        compiler_params=params(8192),
        name="spread",
    )(own, swapped, one_in, two_in, back, send_nodes)


def solution(mesh):
    return jax.shard_map(
        body,
        mesh=mesh,
        in_specs=(P(None, "dom"), P(None, None, "dom"), P(None, "dom"), P(None, "dom"), P()),
        out_specs=P(None, "dom"),
        check_vma=False,
    )
```

```python
import jax
import jax.numpy as jnp
from jax import lax
from jax.experimental import pallas as pl
from jax.experimental.pallas import tpu as pltpu
from jax.sharding import PartitionSpec as P


F32 = jnp.float32
BF16 = jnp.bfloat16
F8 = jnp.float8_e4m3fn
LANES = 128
WIDE = 256
BLK = 512
ELEMS = 4096
NBLK = ELEMS // BLK
NODES = 5632
GHOST = 384
SLOTS = NODES + 8 * GHOST
OWN_ROWS = NODES // WIDE
ALL_ROWS = SLOTS // WIDE
GHOST_ROWS = ALL_ROWS - OWN_ROWS
GHOST_PAD = 16
OWN_PAD = 24
TILES = BLK // LANES
UNROLL = 2
VMEM = pl.BlockSpec(memory_space=pltpu.VMEM)
HBM = pl.BlockSpec(memory_space=pltpu.HBM)


def pad16(n):
    return -(-n // 16) * 16


def iota_rows(rows):
    return lax.broadcasted_iota(jnp.int32, (rows, LANES), 0)


def row_upper(rows, first, count):
    q = iota_rows(count) + first
    u = q
    for s in range(1, 6):
        u = jnp.where(q >= s * rows, q - s * rows, u)
    return jnp.where(q >= 6 * rows, -1, u).astype(F32)


def table_rows(rows):
    return pad16(6 * rows)


def select_parts(rows):
    per = 2 * rows
    out, seen = [], {}
    for g in range(-(-3 * per // 8)):
        for c in sorted({min(8 * g // per, 2), min((8 * g + 7) // per, 2)}):
            key = (max(8 * g, c * per) - c * per, min(8 * g + 8, c * per + per) - c * per, (c * per) % 8)
            if key not in seen:
                upper = row_upper(rows, 8 * g, 8)
                q = iota_rows(8) + 8 * g
                if 8 * g < c * per or 8 * g + 8 > c * per + per:
                    upper = jnp.where((q >= c * per) & (q < c * per + per), upper, -1.0)
                seen[key] = upper
            out.append((g, c, key))
    return out, seen


def select_sums(parts, row, got, lanes):
    order, uppers = parts
    here = jnp.broadcast_to(row, (8, LANES))
    hits, sums = {}, [jnp.zeros((8, LANES), F32)] * 3
    for g, c, key in order:
        if key not in hits:
            hits[key] = uppers[key] == here
        sums[c] = jnp.where(hits[key], got[8 * g:8 * g + 8, lanes:lanes + LANES], sums[c])
    return sums


def fill(tf, rows, x, c, h):
    hi, low = split(x)
    for part, y in ((0, hi), (1, low)):
        tf[pl.ds((c * 2 + part) * rows + h // 2, 1), pl.ds((h % 2) * LANES, LANES)] = y


def lower_parts():
    return [(iota_rows(16) + 16 * g).astype(F32).astype(BF16) for g in range(WIDE // 16)]


def upper_parts(rows):
    return [row_upper(rows, 16 * g, 16).astype(BF16) for g in range(pad16(6 * rows) // 16)]


def wide(row):
    return jnp.broadcast_to(row, (16, LANES)).astype(BF16)


def one_hot(parts, row):
    here, one, zero = wide(row), jnp.ones((16, LANES), BF16), jnp.zeros((16, LANES), BF16)
    return jnp.concatenate([jnp.where(part == here, one, zero) for part in parts], axis=0)


def split(x):
    hi = x.astype(BF16).astype(F32)
    return hi, x - hi


def fold(ref, count):
    for g in range(0, count, 8):
        rows = min(8, count - g)
        total = ref[pl.ds(8 * g, rows, stride=8), :]
        for t in range(1, 8):
            total = total + ref[pl.ds(8 * g + t, rows, stride=8), :]
        yield pl.ds(g, rows), total


def placed(uppers, row, values, rows):
    here, zero = wide(row), jnp.zeros((16, LANES), BF16)
    values = [wide(v) for v in values]
    out = []
    for g, upper in enumerate(uppers):
        first, last = 16 * g // rows, (16 * g + 15) // rows
        value = values[min(first, 5)]
        if last != first and last <= 5:
            cut = (first + 1) * rows - 16 * g
            head = iota_rows(16).astype(F32).astype(BF16) < jnp.full((16, LANES), cut, BF16)
            value = jnp.where(head, value, values[last])
        out.append(jnp.where(upper == here, value, zero))
    return jnp.concatenate(out, axis=0)


def side():
    return lax.rem(lax.axis_index("dom"), 2)


def own_live(live_ref):
    here = lax.broadcasted_iota(jnp.int32, (1, LANES), 1) == lax.axis_index("dom")
    return jnp.sum(jnp.where(here, live_ref[...].astype(F32), 0.0)).astype(jnp.int32)


def by_label(x):
    return jnp.where(side() == 1, pltpu.roll(x, 4, axis=0), x)


def pick_kernel(field_hbm, send_hbm, conn_hbm, live_hbm, swap_ref, out_ref, field_ref, conn_ref, live_ref, send_ref, sem):
    copies = [pltpu.make_async_copy(field_hbm, field_ref, sem.at[0]), pltpu.make_async_copy(send_hbm, send_ref, sem.at[1]),
              pltpu.make_async_copy(conn_hbm, conn_ref, sem.at[2]), pltpu.make_async_copy(live_hbm, live_ref, sem.at[3])]
    for copy in copies:
        copy.start()
    copies[0].wait()
    copies[1].wait()
    place = {0: (swap_ref, 0), 4: (swap_ref, 9), 5: (swap_ref, 18), 6: (swap_ref, 27), 7: (swap_ref, 36),
             1: (out_ref, 0), 2: (out_ref, 9), 3: (out_ref, 18)}
    for j in range(3):
        index = by_label(send_ref[:, pl.ds(j * LANES, LANES)])
        upper, lower = index >> 7, index & 127
        total = [jnp.zeros((8, LANES), F32) for _ in range(3)]
        for h in range(NODES // LANES):
            hit = upper == h
            for c in range(3):
                row = jnp.broadcast_to(field_ref[pl.ds(c, 1), pl.ds(h * LANES, LANES)], (8, LANES))
                total[c] = jnp.where(hit, jnp.take_along_axis(row, lower, axis=1), total[c])
        for c in range(3):
            for m in range(8):
                ref, base = place[m]
                ref[pl.ds(base + c * 3 + j, 1), :] = total[c][m:m + 1, :]
    copies[2].wait()
    copies[3].wait()


def prep_kernel(live_ref, field_ref, conn_ref, after_ref, blocks_hbm, stiff_ref, sums_ref, lo_ref, up_ref, sem, tf):
    del after_ref
    n = own_live(live_ref)

    def fetch(b):
        return pltpu.make_async_copy(blocks_hbm.at[:, :, pl.ds(pl.multiple_of(b * BLK, BLK), BLK)], stiff_ref.at[b], sem.at[b])

    def start(b, _):
        fetch(b).start()
        return 0

    def wait(b, _):
        fetch(b).wait()
        return 0

    lax.fori_loop(0, n, start, 0)
    used = 6 * OWN_ROWS
    tf[pl.ds(used // 8 * 8, tf.shape[0] - used // 8 * 8), :] = jnp.zeros((tf.shape[0] - used // 8 * 8, WIDE), F32)
    for h in range(NODES // LANES):
        x = field_ref[:, pl.ds(h * LANES, LANES)]
        for c in range(3):
            fill(tf, OWN_ROWS, x[c:c + 1, :], c, h)
    table = tf[...].astype(BF16)
    lowers, parts = lower_parts(), select_parts(OWN_ROWS)

    def step(b, _):
        block = pl.ds(pl.multiple_of(b * BLK, BLK), BLK)
        index = conn_ref[:, block]
        lo_ref[b] = (index & (WIDE - 1)).astype(F32)
        up_ref[b] = (index >> 8).astype(F32)
        for a in range(10):
            for t2 in range(TILES // 2):
                cols = [pl.ds((2 * t2 + s) * LANES, LANES) for s in range(2)]
                hot = jnp.concatenate([one_hot(lowers, lo_ref[b, pl.ds(a, 1), c]) for c in cols], axis=1)
                got = jnp.dot(table, hot, preferred_element_type=F32)
                for s in range(2):
                    sums = select_sums(parts, up_ref[b, pl.ds(a, 1), cols[s]], got, s * LANES)
                    for c in range(3):
                        sums_ref[b, (a * TILES + 2 * t2 + s) * 3 + c] = sums[c]
        return 0

    lax.fori_loop(0, n, step, 0)
    lax.fori_loop(0, n, wait, 0)


def main_kernel(live_ref, near_ref, one_ref, two_ref, last_ref, stiff_ref, sums_ref, lo_ref, up_ref,
                swap_ref, one_out_ref, two_out_ref, high_ref, low_ref, tf, vals, high, low, loose_vals, loose_force, total):
    n = own_live(live_ref)
    second = side() == 1

    used = 6 * GHOST_ROWS
    tf[pl.ds(used, tf.shape[0] - used), :] = jnp.zeros((tf.shape[0] - used, WIDE), F32)
    source = {0: (one_ref, 9), 1: (one_ref, 0), 2: (two_ref, 9), 3: (two_ref, 0),
              4: (near_ref, 0), 5: (last_ref, 9), 6: (last_ref, 0), 7: (last_ref, 18)}
    ghost = [source[m][0][pl.ds(source[m][1], 9), :] for m in range(8)]
    for k in range(8):
        bundle = jnp.where(second, ghost[k ^ 4], ghost[k])
        for c in range(3):
            for j in range(3):
                q = c * 3 + j
                fill(tf, GHOST_ROWS, bundle[q:q + 1, :], c, 3 * k + j)
    table = tf[...].astype(BF16)
    total[...] = jnp.zeros_like(total)
    lowers, uppers, parts = lower_parts(), [iota_rows(16).astype(F32).astype(BF16)] * 6, select_parts(GHOST_ROWS)

    def gather(b, half, hots, vals, loose):
        def chunk(a):
            cols = [pl.ds((2 * half + s) * LANES, LANES) for s in range(2)]
            hots[a] = hot = jnp.concatenate([one_hot(lowers, lo_ref[b, pl.ds(a, 1), c]) for c in cols], axis=1).astype(F8)
            got = jnp.dot(table, hot, preferred_element_type=F32)
            for s in range(2):
                sums = select_sums(parts, up_ref[b, pl.ds(a, 1), cols[s]] - OWN_ROWS, got, s * LANES)
                for c in range(3):
                    both = sums[c] + sums_ref[b, (a * TILES + 2 * half + s) * 3 + c]
                    loose[s, pl.ds((c * 10 + a) * 8, 8), :] = both

        def finish():
            for s in range(2):
                for rows, x in fold(loose.at[s], 30):
                    vals[rows, pl.ds(s * LANES, LANES)] = x

        return [lambda a=a: chunk(a) for a in range(10)] + [finish]

    def apply(b, half, vals, high, low, loose):
        def row(i):
            for s in range(2):
                cols = pl.ds(s * LANES, LANES)
                k = stiff_ref[b, i, :, pl.ds((2 * half + s) * LANES, LANES)].astype(F32)
                x = k * vals[:, cols]
                x = x[0:8] + x[8:16] + x[16:24] + jnp.concatenate([x[24:30], jnp.zeros((2, LANES), F32)], axis=0)
                loose[s, pl.ds(8 * i, 8), :] = x

        def finish():
            for s in range(2):
                for rows, x in fold(loose.at[s], 30):
                    high[rows, pl.ds(s * LANES, LANES)] = x
            force = jnp.where(b < n, high[...], 0.0)
            high[...], low[...] = split(force)
            high_ref[b, half], low_ref[b, half] = high[...], low[...]

        return [lambda i=i: row(i) for i in range(30)] + [finish]

    def scatter(b, half, hots, high, low, acc):
        def chunk(a):
            put = []
            for s in range(2):
                cols = pl.ds(s * LANES, LANES)
                values = [ref[pl.ds(c * 10 + a, 1), cols] for c in range(3) for ref in (high, low)]
                row = up_ref[b, pl.ds(a, 1), pl.ds((2 * half + s) * LANES, LANES)] - OWN_ROWS
                put.append(placed(uppers, row, values, GHOST_PAD))
            hot = hots[a]
            part = lax.dot_general(jnp.concatenate(put, axis=1), hot, (((1,), (1,)), ((), ())), preferred_element_type=F32)
            acc[0] = part if acc[0] is None else acc[0] + part

        return [lambda a=a: chunk(a) for a in range(10)]

    def together(*streams):
        pieces = [((i + 1) / len(stream), k, i) for k, stream in enumerate(streams) for i in range(len(stream))]
        for _, k, i in sorted(pieces):
            streams[k][i]()

    def step(trip, _):
        units = [(UNROLL * trip + k, half) for k in range(UNROLL) for half in range(2)]
        hots = [[None] * 10 for _ in units]
        acc = [None]
        buffers = [(vals.at[k], high.at[k], low.at[k]) for k in range(len(units))]
        order = [("gather", k) for k in range(len(units))] + [("apply", 0)]
        for k in range(len(units)):
            order += ([("apply", k + 1)] if k + 1 < len(units) else []) + [("scatter", k)]
        for kind, k in order:
            streams = []
            v, h, w = buffers[k]
            if kind == "scatter":
                streams.append(scatter(*units[k], hots[k], h, w, acc))
            elif kind == "apply":
                streams.append(apply(*units[k], v, h, w, loose_force.at[k]))
            else:
                streams.append(gather(*units[k], hots[k], v, loose_vals.at[k]))
            together(*streams)
        total[...] += acc[0]
        return 0

    lax.fori_loop(0, lax.div(n + (UNROLL - 1), UNROLL), step, 0)

    target = {6: (swap_ref, 0), 5: (swap_ref, 9), 7: (swap_ref, 18), 4: (swap_ref, 27),
              1: (one_out_ref, 0), 0: (one_out_ref, 9), 3: (two_out_ref, 0), 2: (two_out_ref, 9)}

    def partial(k, c, j):
        h = 3 * k + j
        at = 2 * c * GHOST_PAD + h // 2
        cols = pl.ds((h % 2) * LANES, LANES)
        return total[pl.ds(at, 1), cols] + total[pl.ds(at + GHOST_PAD, 1), cols]

    for m in range(4):
        for c in range(3):
            for j in range(3):
                low, high = partial(m, c, j), partial(m + 4, c, j)
                for label, x in ((m, jnp.where(second, high, low)), (m + 4, jnp.where(second, low, high))):
                    ref, base = target[label]
                    ref[pl.ds(base + c * 3 + j, 1), :] = x


def finish_kernel(live_ref, lo_ref, up_ref, high_ref, low_ref, after_ref, own_ref, total):
    del after_ref
    n = own_live(live_ref)
    lowers, uppers = lower_parts(), upper_parts(OWN_PAD)[:3] * 3
    total[...] = jnp.zeros_like(total)

    def step(trip, _):
        acc = None
        for k in range(UNROLL):
            b = UNROLL * trip + k
            for half in range(2):
                for a in range(10):
                    put, hot = [], []
                    for s in range(2):
                        inner, outer = pl.ds(s * LANES, LANES), pl.ds((2 * half + s) * LANES, LANES)
                        hot.append(one_hot(lowers, lo_ref[b, pl.ds(a, 1), outer]))
                        values = [ref[b, half, pl.ds(c * 10 + a, 1), inner] for c in range(3) for ref in (high_ref, low_ref)]
                        put.append(placed(uppers, up_ref[b, pl.ds(a, 1), outer], values, OWN_PAD))
                    part = lax.dot_general(jnp.concatenate(put, axis=1), jnp.concatenate(hot, axis=1).astype(F8),
                                           (((1,), (1,)), ((), ())), preferred_element_type=F32)
                    acc = part if acc is None else acc + part
        total[...] += acc
        return 0

    lax.fori_loop(0, lax.div(n + (UNROLL - 1), UNROLL), step, 0)
    for c in range(3):
        base = 2 * c * OWN_PAD
        own_ref[pl.ds(c * OWN_ROWS, OWN_ROWS), :] = total[pl.ds(base, OWN_ROWS), :] + total[pl.ds(base + OWN_PAD, OWN_ROWS), :]


def spread_kernel(own_ref, swap_ref, one_ref, two_ref, last_ref, send_ref, out_ref, lo, up):
    lowers, uppers = lower_parts(), upper_parts(OWN_ROWS)
    index = by_label(send_ref[...])
    lo[...] = (index & (WIDE - 1)).astype(F32)
    up[...] = (index >> 8).astype(F32)
    source = {0: (swap_ref, 27), 1: (one_ref, 0), 2: (one_ref, 18), 3: (two_ref, 0),
              4: (last_ref, 0), 5: (last_ref, 9), 6: (last_ref, 18), 7: (last_ref, 27)}
    hot, put = [], []
    for m in range(8):
        ref, base = source[m]
        for j in range(3):
            cols = pl.ds(j * LANES, LANES)
            hot.append(one_hot(lowers, lo[pl.ds(m, 1), cols]))
            values = [x for c in range(3) for x in split(ref[pl.ds(base + c * 3 + j, 1), :])]
            put.append(placed(uppers, up[pl.ds(m, 1), cols], values, OWN_ROWS))
    total = None
    for g in range(0, 24, 2):
        part = lax.dot_general(jnp.concatenate(put[g:g + 2], axis=1), jnp.concatenate(hot[g:g + 2], axis=1).astype(F8),
                               (((1,), (1,)), ((), ())), preferred_element_type=F32)
        total = part if total is None else total + part
    for c in range(3):
        for u in range(OWN_ROWS):
            q = 2 * c * OWN_ROWS + u
            out_ref[pl.ds(c, 1), pl.ds(u * WIDE, WIDE)] = (
                total[q:q + 1, :] + total[q + OWN_ROWS:q + OWN_ROWS + 1, :] + own_ref[pl.ds(c * OWN_ROWS + u, 1), :]
            )


def across(x):
    return lax.ppermute(x, "dom", [(i, i ^ 1) for i in range(lax.axis_size("dom"))])


def along(x, o):
    n = lax.axis_size("dom")
    route = {i: i + (2 * o if i % 2 == 0 else -2 * o) for i in range(n)}
    spare = sorted(set(range(n)) - set(route.values()))
    for i in range(n):
        if route[i] not in range(n):
            route[i] = min(spare, key=lambda j: (abs(j - i), j))
            spare.remove(route[i])
    return lax.ppermute(x, "dom", list(route.items()))


def in_hbm(x):
    return pltpu.with_memory_space_constraint(x, pltpu.HBM)


def params(kib):
    return pltpu.CompilerParams(vmem_limit_bytes=kib * 1024)


def rows_f32(*shape):
    return jax.ShapeDtypeStruct(shape, F32)


def prep_call():
    return pl.pallas_call(
        prep_kernel,
        out_shape=(pltpu.VMEM((NBLK, 30, 30, BLK), BF16), pltpu.VMEM((NBLK, 30 * TILES, 8, LANES), F32),
                   pltpu.VMEM((NBLK, 10, BLK), F32), pltpu.VMEM((NBLK, 10, BLK), F32)),
        in_specs=[VMEM] * 4 + [HBM],
        out_specs=(VMEM,) * 4,
        scratch_shapes=[pltpu.SemaphoreType.DMA((NBLK,)), pltpu.VMEM((table_rows(OWN_ROWS), WIDE), F32)],
        compiler_params=params(4096),
        cost_estimate=pl.CostEstimate(flops=2 * 10**10, bytes_accessed=2**23, transcendentals=0),
        name="prep",
    )


def main_call():
    return pl.pallas_call(
        main_kernel,
        out_shape=(rows_f32(36, LANES), rows_f32(18, LANES), rows_f32(18, LANES),
                   pltpu.VMEM((NBLK, 2, 30, BLK // 2), F32), pltpu.VMEM((NBLK, 2, 30, BLK // 2), F32)),
        in_specs=[VMEM] * 9,
        out_specs=(VMEM,) * 5,
        scratch_shapes=[
            pltpu.VMEM((table_rows(GHOST_ROWS), WIDE), F32),
            pltpu.VMEM((2 * UNROLL, 30, BLK // 2), F32),
            pltpu.VMEM((2 * UNROLL, 30, BLK // 2), F32),
            pltpu.VMEM((2 * UNROLL, 30, BLK // 2), F32),
            pltpu.VMEM((2 * UNROLL, 2, 240, LANES), F32),
            pltpu.VMEM((2 * UNROLL, 2, 240, LANES), F32),
            pltpu.VMEM((6 * GHOST_PAD, WIDE), F32),
        ],
        compiler_params=params(16384),
        cost_estimate=pl.CostEstimate(flops=2 * 10**10, bytes_accessed=2**23, transcendentals=0),
        name="main",
    )


def finish_call():
    return pl.pallas_call(
        finish_kernel,
        out_shape=rows_f32(3 * OWN_ROWS, WIDE),
        in_specs=[VMEM] * 6,
        out_specs=VMEM,
        scratch_shapes=[pltpu.VMEM((6 * OWN_PAD, WIDE), F32)],
        compiler_params=params(12288),
        cost_estimate=pl.CostEstimate(flops=2 * 10**10, bytes_accessed=2**23, transcendentals=0),
        name="finish",
    )


def body(field, blocks, connectivity, send_nodes, live_blocks):
    swap, out, field_near, conn_near, live = pl.pallas_call(
        pick_kernel,
        out_shape=(rows_f32(45, LANES), rows_f32(27, LANES), pltpu.VMEM((3, NODES), F32), pltpu.VMEM((10, ELEMS), jnp.int32),
                   pltpu.VMEM((1, LANES), jnp.int32)),
        in_specs=[HBM] * 4,
        out_specs=(VMEM,) * 5,
        scratch_shapes=[pltpu.VMEM((8, GHOST), jnp.int32), pltpu.SemaphoreType.DMA((4,))],
        compiler_params=params(1024),
        name="pick",
    )(in_hbm(field), in_hbm(send_nodes), in_hbm(connectivity), in_hbm(live_blocks.reshape(1, LANES)))
    near = across(swap)
    one = along(jnp.concatenate([out[:9], near[9:18], out[9:18], near[18:27]]), 1)
    two = along(jnp.concatenate([out[18:], near[27:]]), 2)
    last = across(jnp.concatenate([one[18:], two[18:]]))
    stiff, sums, lo, up = prep_call()(live, field_near, conn_near, near, in_hbm(blocks))
    swap, one_out, two_out, high, low = main_call()(live, near, one, two, last, stiff, sums, lo, up)
    swapped = across(swap)
    one_in = along(jnp.concatenate([one_out, swapped[:18]]), -1)
    two_in = along(jnp.concatenate([two_out, swapped[18:27]]), -2)
    own = finish_call()(live, lo, up, high, low, swapped)
    back = across(jnp.concatenate([one_in[9:18], one_in[27:], two_in[9:]]))
    return pl.pallas_call(
        spread_kernel,
        out_shape=rows_f32(3, NODES),
        in_specs=[VMEM] * 6,
        out_specs=VMEM,
        scratch_shapes=[
            pltpu.VMEM((8, GHOST), F32),
            pltpu.VMEM((8, GHOST), F32),
        ],
        compiler_params=params(8192),
        name="spread",
    )(own, swapped, one_in, two_in, back, send_nodes)


def solution(mesh):
    return jax.shard_map(
        body,
        mesh=mesh,
        in_specs=(P(None, "dom"), P(None, None, "dom"), P(None, "dom"), P(None, "dom"), P()),
        out_specs=P(None, "dom"),
        check_vma=False,
    )
```
